32 devices in a mesh: dp: 1 (over z), ty: 4 (over y), tx: 8 (over x, core).
Axes of the slice: x: 4, y: 4, z: 1, core: 2. Of those that a mesh axis runs over, the one named last changes fastest.
The devices are a block of a 4x4x8 slice.
Arguments:
- x: bfloat16 [2048, 8192], P(('dp', 'ty'), 'tx')
- positions: int32 [2, 1024], P('dp')
- norm_gain: float32 [8192], P('tx')
- w_q: bfloat16 [8192, 8192], P('tx', 'ty')
- w_k: bfloat16 [8192, 1024], P('tx', 'ty')
- w_v: bfloat16 [8192, 1024], P('tx', 'ty')
- w_o: bfloat16 [8192, 8192], P('ty', 'tx')
- w_gate: bfloat16 [8192, 24576], P('tx', 'ty')
- w_up: bfloat16 [8192, 24576], P('tx', 'ty')
- w_down: bfloat16 [24576, 8192], P('ty', 'tx')
Outputs:
- output: bfloat16 [2048, 8192], P(('dp', 'ty'), 'tx')
All inputs are finite; a program needn't handle non-finite values.
Results may differ from the reference program's by a relative error of at most 0.0178161.
Values are sent between devices in bfloat16 or wider.
A program may use at most 768 MiB of HBM per device.

```python
import jax
import jax.numpy as jnp
from jax import lax

D = 8192
HEADS = 64
KV_HEADS = 8
FF = 24576
BATCH = 2
SEQ = 1024
HEAD = 128
WINDOW = 4096
ROPE_THETA = 50000
QBLOCK = 256
ROW_BLOCK = 1024

TOKENS = BATCH * SEQ


def setup_inputs(seed: int = 0, part: int = 0) -> dict:
    root_key = jax.random.key(seed)
    shared_keys = jax.random.split(root_key, 8)
    part_keys = jax.random.split(jax.random.fold_in(root_key, part), 7)
    col_frac = jnp.arange(D, dtype=jnp.float32) / D
    wave_freq = jnp.arange(1, 4, dtype=jnp.float32)
    amp_scale = 0.4 * jax.random.normal(part_keys[0], (2, 3), jnp.float32)
    phases = 6.2831853 * jax.random.uniform(part_keys[1], (2, 3), jnp.float32)
    wave_vals = jnp.cos(6.2831853 * wave_freq[None, :, None] * col_frac[None, None, :] + phases[:, :, None])
    col_scale = jnp.exp(jnp.sum(amp_scale[0][:, None] * wave_vals[0], axis=0))
    col_offset = jnp.sum(amp_scale[1][:, None] * wave_vals[1], axis=0)
    tok_mean = jax.random.normal(part_keys[2], (TOKENS, 1), jnp.float32)
    tok_scale = jnp.exp(jax.random.uniform(part_keys[3], (TOKENS, 1), jnp.float32, -0.7, 0.7))
    base_noise = jax.random.normal(part_keys[4], (TOKENS, D), jnp.float32)
    x = (tok_mean + col_offset + tok_scale * col_scale * base_noise).astype(jnp.bfloat16)
    pos_start = jax.random.randint(part_keys[5], (BATCH, 1), 0, 1024)
    pos_gaps = jax.random.randint(part_keys[6], (BATCH, SEQ), 1, 3)
    positions = (pos_start + jnp.cumsum(pos_gaps, axis=1) - 1).astype(jnp.int32)
    norm_gain = 1.0 + 0.3 * jax.random.normal(shared_keys[0], (D,), jnp.float32)

    def draw_weight(key_idx, w_shape, w_scale):
        return (w_scale * jax.random.normal(shared_keys[key_idx], w_shape, jnp.float32)).astype(jnp.bfloat16)

    return {
        "x": x,
        "positions": positions,
        "norm_gain": norm_gain,
        "w_q": draw_weight(1, (D, HEADS * HEAD), 2.0 * D ** -0.5),
        "w_k": draw_weight(2, (D, KV_HEADS * HEAD), D ** -0.5),
        "w_v": draw_weight(3, (D, KV_HEADS * HEAD), D ** -0.5),
        "w_o": draw_weight(4, (HEADS * HEAD, D), 4.0 * (HEADS * HEAD) ** -0.5),
        "w_gate": draw_weight(5, (D, FF), D ** -0.5),
        "w_up": draw_weight(6, (D, FF), D ** -0.5),
        "w_down": draw_weight(7, (FF, D), FF ** -0.5),
    }


def layer_norm(x_rows, norm_gain):
    x_wide = x_rows.astype(jnp.float32)
    tok_mean = jnp.mean(x_wide, axis=-1, keepdims=True)
    centered = x_wide - tok_mean
    tok_var = jnp.mean(centered * centered, axis=-1, keepdims=True)
    return (norm_gain * centered * lax.rsqrt(tok_var + 1e-5)).astype(jnp.bfloat16)


def rotary(heads_in, pos_ids):
    half_dim = HEAD // 2
    inv_freq = ROPE_THETA ** (-2.0 * jnp.arange(half_dim, dtype=jnp.float32) / HEAD)
    rot_angle = pos_ids.astype(jnp.float32)[:, None] * inv_freq[None, :]
    cos_a = jnp.cos(rot_angle)[:, None, :]
    sin_a = jnp.sin(rot_angle)[:, None, :]
    pair_vals = heads_in.astype(jnp.float32).reshape(heads_in.shape[:-1] + (half_dim, 2))
    even_part = pair_vals[..., 0]
    odd_part = pair_vals[..., 1]
    rotated = jnp.stack([even_part * cos_a - odd_part * sin_a, even_part * sin_a + odd_part * cos_a], axis=-1)
    return rotated.reshape(heads_in.shape).astype(jnp.bfloat16)


def attention(q_rot, k_rot, v_heads):
    band_len = min(TOKENS, QBLOCK + min(WINDOW, SEQ))

    def one_block(blk_idx):
        q_start = blk_idx * QBLOCK
        k_start = jnp.clip(q_start + QBLOCK - band_len, 0, TOKENS - band_len)
        q_blk = lax.dynamic_slice_in_dim(q_rot, q_start, QBLOCK, 0)
        k_blk = lax.dynamic_slice_in_dim(k_rot, k_start, band_len, 0)
        v_blk = lax.dynamic_slice_in_dim(v_heads, k_start, band_len, 0)
        scores = jnp.einsum("qgrd,kgd->grqk", q_blk.astype(jnp.float32), k_blk.astype(jnp.float32)) * HEAD ** -0.5
        q_idx = q_start + jnp.arange(QBLOCK)
        k_idx = k_start + jnp.arange(band_len)
        tok_gap = q_idx[:, None] - k_idx[None, :]
        allowed = (tok_gap >= 0) & (tok_gap < WINDOW) & (q_idx[:, None] // SEQ == k_idx[None, :] // SEQ)
        scores = jnp.where(allowed, scores, -1e30)
        row_max = jnp.max(scores, axis=-1, keepdims=True)
        exp_scores = jnp.exp(scores - row_max)
        row_total = jnp.sum(exp_scores, axis=-1)
        weighted = jnp.einsum("grqk,kgd->qgrd", exp_scores.astype(jnp.bfloat16).astype(jnp.float32), v_blk.astype(jnp.float32))
        return (weighted / jnp.transpose(row_total, (2, 0, 1))[..., None]).astype(jnp.bfloat16)

    blocks = lax.map(one_block, jnp.arange(TOKENS // QBLOCK))
    return blocks.reshape(TOKENS, HEADS * HEAD)


def reference(x, positions, norm_gain, w_q, w_k, w_v, w_o, w_gate, w_up, w_down):
    normed = layer_norm(x, norm_gain)
    pos_flat = positions.reshape(TOKENS)
    q_proj = jnp.dot(normed, w_q, preferred_element_type=jnp.float32).astype(jnp.bfloat16)
    k_proj = jnp.dot(normed, w_k, preferred_element_type=jnp.float32).astype(jnp.bfloat16)
    v_proj = jnp.dot(normed, w_v, preferred_element_type=jnp.float32).astype(jnp.bfloat16)
    q_rot = rotary(q_proj.reshape(TOKENS, HEADS, HEAD), pos_flat).reshape(TOKENS, KV_HEADS, HEADS // KV_HEADS, HEAD)
    k_rot = rotary(k_proj.reshape(TOKENS, KV_HEADS, HEAD), pos_flat)
    v_heads = v_proj.reshape(TOKENS, KV_HEADS, HEAD)
    attn_out = attention(q_rot, k_rot, v_heads)

    def row_block(blk_idx):
        row_start = blk_idx * ROW_BLOCK
        n_rows = lax.dynamic_slice_in_dim(normed, row_start, ROW_BLOCK, 0)
        a_rows = lax.dynamic_slice_in_dim(attn_out, row_start, ROW_BLOCK, 0)
        x_rows = lax.dynamic_slice_in_dim(x, row_start, ROW_BLOCK, 0)
        gate_act = jnp.dot(n_rows, w_gate, preferred_element_type=jnp.float32).astype(jnp.bfloat16)
        up_act = jnp.dot(n_rows, w_up, preferred_element_type=jnp.float32).astype(jnp.bfloat16)
        hidden = (jax.nn.silu(gate_act.astype(jnp.float32)) * up_act.astype(jnp.float32)).astype(jnp.bfloat16)
        block_sum = jnp.dot(a_rows, w_o, preferred_element_type=jnp.float32) + jnp.dot(hidden, w_down, preferred_element_type=jnp.float32)
        return (x_rows.astype(jnp.float32) + block_sum).astype(jnp.bfloat16)

    y_out = lax.map(row_block, jnp.arange(TOKENS // ROW_BLOCK))
    return y_out.reshape(TOKENS, D)
```

```python
import functools
import math
import jax
import jax.numpy as jnp
from jax import lax
from jax.experimental import pallas as pl
from jax.experimental.pallas import tpu as pltpu
from jax.sharding import PartitionSpec as P

HEAD = 128
WINDOW = 4096
ROPE_THETA = 50000
QBLOCK = 256
CORES = 2
MESH = pl.DeviceIdType.MESH
F32 = jnp.float32
BF16 = jnp.bfloat16


def rotary(heads_in, pos_ids):
    half_dim = HEAD // 2
    inv_freq = ROPE_THETA ** (-2.0 * jnp.arange(half_dim, dtype=jnp.float32) / HEAD)
    rot_angle = pos_ids.astype(jnp.float32)[:, None] * inv_freq[None, :]
    cos_a = jnp.cos(rot_angle)[:, None, :]
    sin_a = jnp.sin(rot_angle)[:, None, :]
    pair_vals = heads_in.astype(jnp.float32).reshape(heads_in.shape[:-1] + (half_dim, 2))
    even_part = pair_vals[..., 0]
    odd_part = pair_vals[..., 1]
    rotated = jnp.stack([even_part * cos_a - odd_part * sin_a, even_part * sin_a + odd_part * cos_a], axis=-1)
    return rotated.reshape(heads_in.shape).astype(jnp.bfloat16)


def band_attention(q_rot, k_rot, v_heads, q_first, seq_len):
    q_rows = q_rot.shape[0]
    tokens = k_rot.shape[0]
    q_block = math.gcd(q_rows, QBLOCK)
    band_len = min(tokens, q_block + min(WINDOW, seq_len))
    q_blocks = q_rot.reshape((q_rows // q_block, q_block) + q_rot.shape[1:])

    def one_block(blk_args):
        q_blk, blk_idx = blk_args
        q_start = q_first + blk_idx * q_block
        k_start = jnp.clip(q_start + q_block - band_len, 0, tokens - band_len)
        k_blk = lax.dynamic_slice_in_dim(k_rot, k_start, band_len, 0)
        v_blk = lax.dynamic_slice_in_dim(v_heads, k_start, band_len, 0)
        scores = jnp.einsum("qgrd,kgd->grqk", q_blk, k_blk, preferred_element_type=jnp.float32) * HEAD ** -0.5
        q_idx = q_start + jnp.arange(q_block)
        k_idx = k_start + jnp.arange(band_len)
        tok_gap = q_idx[:, None] - k_idx[None, :]
        allowed = (tok_gap >= 0) & (tok_gap < WINDOW) & (q_idx[:, None] // seq_len == k_idx[None, :] // seq_len)
        scores = jnp.where(allowed, scores, -1e30)
        row_max = jnp.max(scores, axis=-1, keepdims=True)
        exp_scores = jnp.exp(scores - row_max)
        row_total = jnp.sum(exp_scores, axis=-1)
        weighted = jnp.einsum("grqk,kgd->qgrd", exp_scores.astype(jnp.bfloat16), v_blk, preferred_element_type=jnp.float32)
        return (weighted / jnp.transpose(row_total, (2, 0, 1))[..., None]).astype(jnp.bfloat16)

    results = lax.map(one_block, (q_blocks, jnp.arange(q_rows // q_block)))
    return results.reshape(q_rows, -1)


def swap_kernel(wg, wu, wd, wgp, wup, wdp, send_sem, recv_sem):
    half = wgp.shape[1]
    tx = lax.axis_index("tx")
    core = lax.rem(tx, CORES)
    partner = tx + 1 - 2 * core
    barrier = pltpu.get_barrier_semaphore()
    pl.semaphore_signal(barrier, inc=1, device_id={"tx": partner}, device_id_type=MESH)
    pl.semaphore_wait(barrier, 1)
    off = pl.multiple_of((1 - core) * half, 128)
    copies = []
    for i, (src, dst) in enumerate(((wg.at[:, pl.ds(off, half)], wgp), (wu.at[:, pl.ds(off, half)], wup),
                                    (wd.at[pl.ds(off, half), :], wdp))):
        copies.append(pltpu.make_async_remote_copy(src_ref=src, dst_ref=dst, send_sem=send_sem.at[i], recv_sem=recv_sem.at[i],
                                                   device_id={"tx": partner}, device_id_type=MESH))
        copies[-1].start()
    for copy in copies:
        copy.wait()


def swap_weights(wg, wu, wd):
    half = wg.shape[1] // CORES
    any_spec = pl.BlockSpec(memory_space=pl.ANY)
    return pl.pallas_call(
        swap_kernel,
        out_shape=(jax.ShapeDtypeStruct((wg.shape[0], half), BF16), jax.ShapeDtypeStruct((wg.shape[0], half), BF16),
                   jax.ShapeDtypeStruct((half, wd.shape[1]), BF16)),
        in_specs=[any_spec] * 3, out_specs=[any_spec] * 3,
        scratch_shapes=[pltpu.SemaphoreType.DMA((3,)), pltpu.SemaphoreType.DMA((3,))],
        compiler_params=pltpu.CompilerParams(collective_id=0, has_side_effects=True, vmem_limit_bytes=4 << 20),
    )(wg, wu, wd)


SLOTS = 3
HSLOTS = 8


def mlp_kernel(nx, ny, width, n_hbm, base_hbm, wg, wu, wgp, wup, wd, wdp, out_ref,
               nown, npar, wbuf, w2buf, pbuf, sbuf, rbuf, hid, acc, xrecv, ysend, yrecv,
               in_sem, w_sem, w2_sem, send_sem, recv_sem, xs_sem, xr_sem, ys_sem, yr_sem, nx_sems, credit, xcredit):
    tokens, feats = nown.shape
    bt = tokens // ny
    ob = bt // nx
    half = wgp.shape[1]
    dircols = half // 2
    chunks = dircols // width
    total = ny * chunks
    last_hop = nx - 1
    kinds = 2 * last_hop
    tx = lax.axis_index("tx")
    ty = lax.axis_index("ty")
    core = lax.rem(tx, CORES)
    pos = tx // CORES
    partner = tx + 1 - 2 * core

    def target(d):
        return lax.rem(pos + 1 + d * (nx - 2), nx) * CORES + core

    def source(d):
        return lax.rem(pos + nx - 1 - d * (nx - 2), nx) * CORES + core

    def owner_rows(d, step):
        o = lax.rem(pos + (nx - 1 - step if d == 0 else 1 + step), nx)
        return pl.ds(pl.multiple_of(o * ob, ob), ob)

    def gather_rows(d, hops):
        o = lax.rem(pos + (nx - hops if d == 0 else hops), nx)
        return pl.ds(pl.multiple_of(o * ob, ob), ob)

    def block_rows(p):
        return pl.ds(pl.multiple_of(lax.rem(ty + 1 + p, ny) * bt, bt), bt)

    barrier = pltpu.get_barrier_semaphore()
    peers = [{"tx": partner}, {"tx": target(0)}, {"tx": target(1)}] + [{"ty": lax.rem(ty + k, ny)} for k in range(1, ny)]
    for peer in peers:
        pl.semaphore_signal(barrier, inc=1, device_id=peer, device_id_type=MESH)

    def w_copies(q, d):
        slot = lax.rem(q, 2)
        j = lax.rem(q, chunks)
        own = pl.ds(pl.multiple_of(core * half + d * dircols + j * width, width), width)
        par = pl.ds(pl.multiple_of(d * dircols + j * width, width), width)
        top, low = pl.ds(0, feats), pl.ds(feats, feats)
        left, right = pl.ds(0, width), pl.ds(width, width)
        dst = wbuf.at[slot, d]
        sem = w_sem.at[slot, d]
        return (pltpu.make_async_copy(wg.at[:, own], dst.at[top, left], sem.at[0]),
                pltpu.make_async_copy(wu.at[:, own], dst.at[top, right], sem.at[1]),
                pltpu.make_async_copy(wgp.at[:, par], dst.at[low, left], sem.at[2]),
                pltpu.make_async_copy(wup.at[:, par], dst.at[low, right], sem.at[3]))

    def w2_copies(q, d):
        slot = lax.rem(q, 2)
        j = lax.rem(q, chunks)
        own = pl.ds(pl.multiple_of(core * half + d * dircols + j * width, width), width)
        par = pl.ds(pl.multiple_of(d * dircols + j * width, width), width)
        dst = w2buf.at[slot]
        rows = pl.ds(d * width, width)
        sem = w2_sem.at[slot, d]
        return (pltpu.make_async_copy(wd.at[own, :], dst.at[0, rows, :], sem.at[0]),
                pltpu.make_async_copy(wdp.at[par, :], dst.at[1, rows, :], sem.at[1]))

    def start(copies):
        for copy in copies:
            copy.start()

    def wait(copies):
        for copy in copies:
            copy.wait()

    def hop(k, d, t):
        slot = lax.rem(t, SLOTS)
        if k < last_hop:
            src, dst = sbuf.at[d, k, slot], rbuf.at[d, k, slot]
        else:
            hslot = lax.rem(t - k + HSLOTS, HSLOTS)
            rows = gather_rows(d, k - last_hop)
            src = dst = hid.at[d, hslot, rows, :]
        return pltpu.make_async_remote_copy(src_ref=src, dst_ref=dst, send_sem=send_sem.at[d, k, slot],
                                            recv_sem=recv_sem.at[d, k, slot], device_id={"tx": target(d)}, device_id_type=MESH)

    def arrival(k, d, t):
        slot = lax.rem(t - 1 + SLOTS, SLOTS)
        if k < last_hop:
            dst = rbuf.at[d, k, slot]
        else:
            hslot = lax.rem(t - 1 - k + HSLOTS, HSLOTS)
            dst = hid.at[d, hslot, gather_rows(d, k - last_hop + 1), :]
        pltpu.make_async_remote_copy(src_ref=dst, dst_ref=dst, send_sem=send_sem.at[d, k, slot], recv_sem=recv_sem.at[d, k, slot],
                                     device_id={"tx": target(d)}, device_id_type=MESH).wait_recv()

    def valid(q):
        return jnp.logical_and(q >= 0, q < total)

    for d in range(2):
        start(w_copies(0, d))
    load_n = pltpu.make_async_copy(n_hbm, nown, in_sem.at[0])
    load_n.start()
    pl.semaphore_wait(barrier, len(peers))
    load_n.wait()
    swap_n = pltpu.make_async_remote_copy(src_ref=nown, dst_ref=npar, send_sem=nx_sems.at[0], recv_sem=nx_sems.at[1],
                                          device_id={"tx": partner}, device_id_type=MESH)
    swap_n.start()
    swap_n.wait()

    sends = total + kinds - 1
    signal_end = sends - SLOTS + 1

    def exchange_copy():
        return pltpu.make_async_remote_copy(src_ref=acc.at[1], dst_ref=xrecv, send_sem=xs_sem, recv_sem=xr_sem,
                                            device_id={"tx": partner}, device_id_type=MESH)

    def y_copy(p):
        return pltpu.make_async_remote_copy(src_ref=ysend.at[p], dst_ref=yrecv.at[p], send_sem=ys_sem.at[p], recv_sem=yr_sem.at[p],
                                            device_id={"ty": lax.rem(ty + 1 + p, ny)}, device_id_type=MESH)

    def tick(t, carry):
        @pl.when(jnp.logical_and(t >= SLOTS, t < sends))
        def _():
            for d in range(2):
                pl.semaphore_wait(credit.at[d], 1)

        for k in range(kinds):
            @pl.when(valid(t - SLOTS - k))
            def _():
                for d in range(2):
                    hop(k, d, t - SLOTS).wait_send()

        @pl.when(t < total)
        def _():
            for d in range(2):
                wait(w_copies(t, d))

            @pl.when(t + 1 < total)
            def _():
                for d in range(2):
                    start(w_copies(t + 1, d))

            rows = block_rows(t // chunks)
            slot = lax.rem(t, 2)
            pslot = lax.rem(t, nx)

            @pl.loop(0, 2)
            def _(d):
                pbuf[d, pslot] = (jnp.dot(nown[rows, :], wbuf[slot, d, :feats, :], preferred_element_type=F32)
                                  + jnp.dot(npar[rows, :], wbuf[slot, d, feats:, :], preferred_element_type=F32))
            for d in range(2):
                sbuf[d, 0, lax.rem(t, SLOTS)] = pbuf[d, pslot, owner_rows(d, 0), :].astype(BF16)
                hop(0, d, t).start()

        for k in range(1, last_hop + 1):
            @pl.when(valid(t - k))
            def _():
                for d in range(2):
                    arrival(k - 1, d, t)
                    part = (pbuf[d, lax.rem(t - k + nx, nx), owner_rows(d, k), :]
                            + rbuf[d, k - 1, lax.rem(t - 1 + SLOTS, SLOTS)].astype(F32))
                    if k < last_hop:
                        sbuf[d, k, lax.rem(t, SLOTS)] = part.astype(BF16)
                    else:
                        gate = part[:, :width].astype(BF16).astype(F32)
                        up = part[:, width:].astype(BF16).astype(F32)
                        hslot = lax.rem(t - k + HSLOTS, HSLOTS)
                        hid[d, hslot, gather_rows(d, 0), :] = (gate * jax.nn.sigmoid(gate) * up).astype(BF16)
                    hop(k, d, t).start()

        for k in range(last_hop + 1, kinds):
            @pl.when(valid(t - k))
            def _():
                for d in range(2):
                    arrival(k - 1, d, t)
                    hop(k, d, t).start()

        q = t - kinds

        prev = q - 1

        @pl.when(jnp.logical_and(valid(prev), lax.rem(prev + 1, chunks) == 0))
        def _():
            p = prev // chunks
            copy = exchange_copy()
            copy.wait()

            @pl.when(p < ny - 1)
            def _():
                ysend[p] = (acc[0] + xrecv[...]).astype(BF16)
                pl.semaphore_signal(xcredit, inc=1, device_id={"tx": partner}, device_id_type=MESH)
                y_copy(p).start()

            @pl.when(p == ny - 1)
            def _():
                out = acc[0] + xrecv[...]
                for i in range(ny - 1):
                    y_copy(i).wait_recv()
                    out += yrecv[i].astype(F32)
                acc[0] = out

        @pl.when(valid(q))
        def _():
            p = q // chunks

            @pl.when(lax.rem(q, chunks) == 0)
            def _():
                load = pltpu.make_async_copy(base_hbm.at[block_rows(p), :], acc.at[0], in_sem.at[0])
                load.start()
                acc[1] = jnp.zeros_like(acc[1])
                load.wait()

            for d in range(2):
                wait(w2_copies(q, d))
                arrival(kinds - 1, d, t)

            hslot = lax.rem(q, HSLOTS)
            slot = lax.rem(q, 2)

            @pl.loop(0, 2)
            def _(o):
                acc[o] += (jnp.dot(hid[0, hslot], w2buf[slot, o, :width, :], preferred_element_type=F32)
                           + jnp.dot(hid[1, hslot], w2buf[slot, o, width:, :], preferred_element_type=F32))

            @pl.when(lax.rem(q + 1, chunks) == 0)
            def _():
                @pl.when(p > 0)
                def _():
                    pl.semaphore_wait(xcredit, 1)
                exchange_copy().start()

        @pl.when(valid(q + 1))
        def _():
            for d in range(2):
                start(w2_copies(q + 1, d))

        @pl.when(jnp.logical_and(t >= 1, t < signal_end))
        def _():
            for d in range(2):
                pl.semaphore_signal(credit.at[d], inc=1, device_id={"tx": source(d)}, device_id_type=MESH)
        return carry

    lax.fori_loop(0, total + kinds - 1 + SLOTS, tick, 0)
    for i in range(ny - 1):
        y_copy(i).wait_send()
    store = pltpu.make_async_copy(acc.at[0], out_ref, in_sem.at[0])
    store.start()
    store.wait()


def mlp_ring(n_all, base, wg, wu, wgp, wup, wd, wdp, nx, ny, width):
    tokens, feats = n_all.shape
    bt = tokens // ny
    ob = bt // nx
    cols = wd.shape[1]
    kinds = 2 * (nx - 1)
    any_spec = pl.BlockSpec(memory_space=pl.ANY)
    dma = pltpu.SemaphoreType.DMA
    return pl.pallas_call(
        functools.partial(mlp_kernel, nx, ny, width),
        out_shape=jax.ShapeDtypeStruct((bt, cols), F32),
        in_specs=[any_spec] * 8, out_specs=any_spec,
        scratch_shapes=[
            pltpu.VMEM((tokens, feats), BF16),
            pltpu.VMEM((tokens, feats), BF16),
            pltpu.VMEM((2, 2, 2 * feats, 2 * width), BF16),
            pltpu.VMEM((2, 2, 2 * width, cols), BF16),
            pltpu.VMEM((2, nx, bt, 2 * width), F32),
            pltpu.VMEM((2, nx - 1, SLOTS, ob, 2 * width), BF16),
            pltpu.VMEM((2, nx - 1, SLOTS, ob, 2 * width), BF16),
            pltpu.VMEM((2, HSLOTS, bt, width), BF16),
            pltpu.VMEM((2, bt, cols), F32),
            pltpu.VMEM((bt, cols), F32),
            pltpu.VMEM((ny - 1, bt, cols), BF16),
            pltpu.VMEM((ny - 1, bt, cols), BF16),
            dma((1,)), dma((2, 2, 4)), dma((2, 2, 2)),
            dma((2, kinds, SLOTS)), dma((2, kinds, SLOTS)),
            dma, dma, dma((ny - 1,)), dma((ny - 1,)), dma((2,)),
            pltpu.SemaphoreType.REGULAR((2,)), pltpu.SemaphoreType.REGULAR,
        ],
        compiler_params=pltpu.CompilerParams(collective_id=1, has_side_effects=True, vmem_limit_bytes=67043328),
        cost_estimate=pl.CostEstimate(flops=400_000_000_000, bytes_accessed=200_000_000, transcendentals=0),
    )(n_all, base, wg, wu, wgp, wup, wd, wdp)


def solution(mesh):
    tx_size = mesh.shape["tx"]
    ty_size = mesh.shape["ty"]

    def per_device(x_blk, positions, norm_gain, w_q, w_k, w_v, w_o, w_gate, w_up, w_down):
        d_model = x_blk.shape[1] * tx_size
        seq_len = positions.shape[1]
        wgp, wup, wdp = swap_weights(w_gate, w_up, w_down)
        x_wide = x_blk.astype(jnp.float32)
        tok_stats = lax.psum(jnp.stack([jnp.sum(x_wide, axis=1), jnp.sum(x_wide * x_wide, axis=1)], axis=1), "tx")
        tok_mean = tok_stats[:, :1] / d_model
        tok_var = tok_stats[:, 1:] / d_model - tok_mean * tok_mean
        normed = (norm_gain * (x_wide - tok_mean) * lax.rsqrt(tok_var + 1e-5)).astype(jnp.bfloat16)
        n_all = lax.all_gather(normed, "ty", axis=0, tiled=True)
        tokens = n_all.shape[0]
        q_rows = tokens // tx_size
        part_q = jnp.dot(n_all, w_q, preferred_element_type=jnp.float32).astype(jnp.bfloat16)
        part_rest = tuple(jnp.dot(n_all, w_mat, preferred_element_type=jnp.float32).astype(jnp.bfloat16) for w_mat in (w_k, w_v))
        q_proj = lax.psum_scatter(part_q, "tx", scatter_dimension=0, tiled=True)
        k_proj, v_proj = lax.psum(part_rest, "tx")
        heads_loc = w_q.shape[1] // HEAD
        kv_loc = k_proj.shape[1] // HEAD
        pos_flat = positions.reshape(tokens)
        q_first = lax.axis_index("tx") * q_rows
        q_pos = lax.dynamic_slice_in_dim(pos_flat, q_first, q_rows, 0)
        q_rot = rotary(q_proj.reshape(q_rows, heads_loc, HEAD), q_pos).reshape(q_rows, kv_loc, heads_loc // kv_loc, HEAD)
        k_rot = rotary(k_proj.reshape(tokens, kv_loc, HEAD), pos_flat)
        v_heads = v_proj.reshape(tokens, kv_loc, HEAD)
        attn_rows = band_attention(q_rot, k_rot, v_heads, q_first, seq_len)
        attn_all = lax.all_gather(attn_rows, "tx", axis=0, tiled=True)
        base = jnp.dot(attn_all, w_o, preferred_element_type=jnp.float32)
        block_sum = mlp_ring(n_all, base, w_gate, w_up, wgp, wup, w_down, wdp, tx_size // CORES, ty_size, 256)
        return (x_wide + block_sum).astype(jnp.bfloat16)

    in_specs = (P(("dp", "ty"), "tx"), P("dp", None), P("tx"), P("tx", "ty"), P("tx", "ty"), P("tx", "ty"),
                P("ty", "tx"), P("tx", "ty"), P("tx", "ty"), P("ty", "tx"))
    return jax.shard_map(per_device, mesh=mesh, in_specs=in_specs, out_specs=P(("dp", "ty"), "tx"), check_vma=False)
```

```python
import functools
import jax
import jax.numpy as jnp
from jax import lax
from jax.experimental import pallas as pl
from jax.experimental.pallas import tpu as pltpu
from jax.sharding import PartitionSpec as P

HEAD = 128
WINDOW = 4096
ROPE_THETA = 50000
CORES = 2
MESH = pl.DeviceIdType.MESH
F32 = jnp.float32
BF16 = jnp.bfloat16


def swap_lanes(x):
    width = x.shape[1]
    even = lax.rem(lax.broadcasted_iota(jnp.int32, x.shape, 1), 2) == 0
    return jnp.where(even, pltpu.roll(x, width - 1, 1), pltpu.roll(x, 1, 1))


def qkv_kernel(nx, ny, n_hbm, cos_ref, sin_ref, wq, wk, wv, wg, wu, nown_out, npar_out, q_out, kv_out, wgp, wup,
               nown, npar, wbuf, pbuf, sbuf, rbuf, qst, kv, in_sem, w_sem, ws_sem, wr_sem, ns_sem, nr_sem, ps_sem, pr_sem,
               send_sem, recv_sem, ks_sem, kr_sem, gs_sem, gr_sem):
    tokens, feats = nown.shape
    bt = tokens // ny
    hb = bt // 2
    ob = bt // nx
    half = wgp.shape[1]
    qcols = wq.shape[1] // CORES // 2
    hops = nx - 1
    order = (0, 1, 3, 2)
    tx = lax.axis_index("tx")
    ty = lax.axis_index("ty")
    core = lax.rem(tx, CORES)
    pos = tx // CORES
    partner = tx + 1 - 2 * core
    north, south = lax.rem(ty + 1, ny), lax.rem(ty + ny - 1, ny)

    def chip(i):
        return lax.rem(pos + i, nx) * CORES + core

    def owner_rows(d, step):
        o = lax.rem(pos + (nx - 1 - step if d == 0 else 1 + step), nx)
        return pl.ds(pl.multiple_of(o * ob, ob), ob)

    def rows_of(off):
        return pl.ds(pl.multiple_of(lax.rem(ty + off, ny) * bt, bt), bt)

    def half_rows(off, i):
        return pl.ds(pl.multiple_of(lax.rem(ty + off, ny) * bt + i * hb, hb), hb)

    def remote(src, dst, send, recv, device):
        return pltpu.make_async_remote_copy(src_ref=src, dst_ref=dst, send_sem=send, recv_sem=recv, device_id=device, device_id_type=MESH)

    barrier = pltpu.get_barrier_semaphore()
    peers = [{"tx": partner}] + [{"tx": chip(i)} for i in range(1, nx)] + [{"ty": lax.rem(ty + k, ny)} for k in range(1, ny)]
    for peer in peers:
        pl.semaphore_signal(barrier, inc=1, device_id=peer, device_id_type=MESH)

    load_n = pltpu.make_async_copy(n_hbm, nown.at[rows_of(0), :], in_sem.at[0])
    load_n.start()

    def w_parts(c):
        parts = []
        for d in range(2):
            col = pl.ds(pl.multiple_of(c * 2 * qcols + d * qcols, 128), qcols)
            small = pl.ds(pl.multiple_of(c * HEAD, HEAD), HEAD)
            parts.append((wq.at[:, col], d, pl.ds(0, qcols)))
            parts.append(((wk if d == 0 else wv).at[:, small], d, pl.ds(qcols, HEAD)))
        return parts

    local_w = [pltpu.make_async_copy(s, wbuf.at[d, pl.ds(0, feats), cols], w_sem.at[i]) for i, (s, d, cols) in enumerate(w_parts(core))]
    for copy in local_w:
        copy.start()
    pl.semaphore_wait(barrier, len(peers))
    load_n.wait()

    own = nown.at[rows_of(0), :]
    swap_w = [remote(s, wbuf.at[d, pl.ds(feats, feats), cols], ws_sem.at[i], wr_sem.at[i], {"tx": partner})
              for i, (s, d, cols) in enumerate(w_parts(1 - core))]
    to_south = remote(own, own, ns_sem.at[0], nr_sem.at[0], {"ty": south})
    to_north = remote(own, own, ns_sem.at[1], nr_sem.at[1], {"ty": north})
    to_south.start()
    to_north.start()

    def pair(p):
        rows = rows_of(order[p])
        return remote(nown.at[rows, :], npar.at[rows, :], ps_sem.at[p], pr_sem.at[p], {"tx": partner})

    def far(i):
        rows = half_rows(1 if i == 0 else ny - 1, i)
        return remote(nown.at[rows, :], nown.at[rows, :], ns_sem.at[2 + i], nr_sem.at[2 + i], {"ty": south if i == 0 else north})

    def far_arrival(i):
        rows = half_rows(2, i)
        return remote(nown.at[rows, :], nown.at[rows, :], ns_sem.at[2 + i], nr_sem.at[2 + i], {"ty": south if i == 0 else north})

    def near_arrival(i):
        rows = rows_of(1 if i == 0 else ny - 1)
        return remote(nown.at[rows, :], nown.at[rows, :], ns_sem.at[i], nr_sem.at[i], {"ty": south if i == 0 else north})

    pair(0).start()
    for copy in swap_w:
        copy.start()

    piece = feats // ny
    goff = pl.multiple_of((1 - core) * half, 128)

    def swap_mlp(i):
        rows = pl.ds(i * piece, piece)
        return [remote(src.at[rows, pl.ds(goff, half)], dst.at[rows, :], gs_sem.at[k, i], gr_sem.at[k, i], {"tx": partner})
                for k, (src, dst) in enumerate(((wg, wgp), (wu, wup)))]

    def hop(k, d, p):
        target = chip(1 if d == 0 else nx - 1)
        return remote(sbuf.at[d, k, p], rbuf.at[d, k, p], send_sem.at[d, k, p], recv_sem.at[d, k, p], {"tx": target})

    def kv_rows(p):
        return pl.ds(pl.multiple_of(lax.rem(ty + order[p], ny) * bt + pos * ob, ob), ob)

    def kv_copy(d, p, i):
        rows = kv_rows(p)
        return remote(kv.at[d, rows, :], kv.at[d, rows, :], ks_sem.at[d, p, i - 1], kr_sem.at[d, p, i - 1], {"tx": chip(i)})

    def kv_arrival(d, p, i):
        rows = pl.ds(pl.multiple_of(lax.rem(ty + order[p], ny) * bt + lax.rem(pos + nx - i, nx) * ob, ob), ob)
        return remote(kv.at[d, rows, :], kv.at[d, rows, :], ks_sem.at[d, p, i - 1], kr_sem.at[d, p, i - 1], {"tx": chip(i)})

    def n_store(p):
        rows = rows_of(order[p])
        return (pltpu.make_async_copy(nown.at[rows, :], nown_out.at[rows, :], in_sem.at[1 + 2 * p]),
                pltpu.make_async_copy(npar.at[rows, :], npar_out.at[rows, :], in_sem.at[2 + 2 * p]))

    for t in range(ny + hops):
        if t < ny:
            if t == 1:
                near_arrival(0).wait_recv()
                far(0).start()
                pair(1).start()
                near_arrival(1).wait_recv()
                far(1).start()
                pair(2).start()
            if t == 3:
                far_arrival(0).wait_recv()
                far_arrival(1).wait_recv()
                pair(3).start()
            pair(t).wait_recv()
            for copy in n_store(t):
                copy.start()
            if t == 0:
                for copy in local_w:
                    copy.wait()
                for copy in swap_w:
                    copy.wait_recv()
            rows = rows_of(order[t])

            @pl.loop(0, 2)
            def _(d):
                pbuf[d, t % nx] = (jnp.dot(nown[rows, :], wbuf[d, :feats, :], preferred_element_type=F32)
                                   + jnp.dot(npar[rows, :], wbuf[d, feats:, :], preferred_element_type=F32))
            for d in range(2):
                sbuf[d, 0, t] = pbuf[d, t % nx, owner_rows(d, 0), :].astype(BF16)
                hop(0, d, t).start()
            for copy in swap_mlp(t):
                copy.start()
        for k in range(1, hops + 1):
            p = t - k
            if 0 <= p < ny:
                for d in range(2):
                    hop(k - 1, d, p).wait_recv()
                    part = pbuf[d, p % nx, owner_rows(d, k), :] + rbuf[d, k - 1, p].astype(F32)
                    if k < hops:
                        sbuf[d, k, p] = part.astype(BF16)
                        hop(k, d, p).start()
                        continue
                    rows = kv_rows(p)
                    block = lax.rem(ty + order[p], ny)
                    part = part.astype(BF16).astype(F32)
                    cos, sin = cos_ref[rows, :], sin_ref[rows, :]
                    small = part[:, qcols:]
                    if d == 0:
                        small = small * cos + swap_lanes(small) * sin
                    kv[d, rows, :] = small.astype(BF16)
                    for i in range(1, nx):
                        kv_copy(d, p, i).start()
                    for h in range(qcols // HEAD):
                        head = part[:, h * HEAD:(h + 1) * HEAD]
                        qst[block, :, d * qcols + h * HEAD:d * qcols + (h + 1) * HEAD] = (head * cos + swap_lanes(head) * sin).astype(BF16)

    for p in range(ny):
        for d in range(2):
            for i in range(1, nx):
                kv_arrival(d, p, i).wait_recv()
                kv_copy(d, p, i).wait_send()
            for k in range(hops):
                hop(k, d, p).wait_send()
        pair(p).wait_send()
        for copy in n_store(p):
            copy.wait()
        for copy in swap_mlp(p):
            copy.wait()
    for copy in swap_w:
        copy.wait_send()
    to_south.wait_send()
    to_north.wait_send()
    far(0).wait_send()
    far(1).wait_send()
    stores = (pltpu.make_async_copy(qst, q_out, in_sem.at[0]), pltpu.make_async_copy(kv, kv_out, in_sem.at[1]))
    for copy in stores:
        copy.start()
    for copy in stores:
        copy.wait()


def qkv_ring(n_blk, cos, sin, wq, wk, wv, wg, wu, nx, ny):
    bt, feats = n_blk.shape
    tokens = bt * ny
    ob = bt // nx
    half = wg.shape[1] // CORES
    qhalf = wq.shape[1] // CORES
    cols = qhalf // 2 + HEAD
    hops = nx - 1
    any_spec = pl.BlockSpec(memory_space=pl.ANY)
    vmem = pl.BlockSpec(memory_space=pltpu.VMEM)
    dma = pltpu.SemaphoreType.DMA
    sds = jax.ShapeDtypeStruct
    return pl.pallas_call(
        functools.partial(qkv_kernel, nx, ny),
        out_shape=(sds((tokens, feats), BF16), sds((tokens, feats), BF16), sds((ny, ob, qhalf), BF16), sds((2, tokens, HEAD), BF16),
                   sds((feats, half), BF16), sds((feats, half), BF16)),
        in_specs=[any_spec, vmem, vmem] + [any_spec] * 5, out_specs=[any_spec] * 6,
        scratch_shapes=[
            pltpu.VMEM((tokens, feats), BF16), pltpu.VMEM((tokens, feats), BF16),
            pltpu.VMEM((2, 2 * feats, cols), BF16),
            pltpu.VMEM((2, nx, bt, cols), F32),
            pltpu.VMEM((2, hops, ny, ob, cols), BF16), pltpu.VMEM((2, hops, ny, ob, cols), BF16),
            pltpu.VMEM((ny, ob, qhalf), BF16), pltpu.VMEM((2, tokens, HEAD), BF16),
            dma((1 + 2 * ny,)), dma((4,)), dma((4,)), dma((4,)), dma((4,)), dma((4,)), dma((ny,)), dma((ny,)),
            dma((2, hops, ny)), dma((2, hops, ny)), dma((2, ny, hops)), dma((2, ny, hops)), dma((2, ny)), dma((2, ny)),
        ],
        compiler_params=pltpu.CompilerParams(collective_id=0, has_side_effects=True, vmem_limit_bytes=60 << 20),
        cost_estimate=pl.CostEstimate(flops=60_000_000_000, bytes_accessed=60_000_000, transcendentals=0),
    )(n_blk, cos, sin, wq, wk, wv, wg, wu)


SLOTS = 3
HSLOTS = 8


def mlp_kernel(nx, ny, width, seq_len, nown_hbm, npar_hbm, q_hbm, kv_hbm, wg, wu, wgp, wup, wd, wo, out_ref, wdp, wop,
               nown, npar, wbuf, w2buf, pbuf, sbuf, rbuf, hid, acc, xrecv, ysend, yrecv, qst, kv, abuf,
               in_sem, n_sem, w_sem, w2_sem, send_sem, recv_sem, xs_sem, xr_sem, ys_sem, yr_sem, gs_sem, gr_sem, credit, xcredit):
    tokens, feats = nown.shape
    bt = tokens // ny
    ob = bt // nx
    half = wgp.shape[1]
    dircols = half // 2
    ahalf = wop.shape[0]
    adir = ahalf // 2
    mlp_chunks = dircols // width
    chunks = mlp_chunks + adir // width
    total = ny * chunks
    last_hop = nx - 1
    kinds = 2 * last_hop
    tx = lax.axis_index("tx")
    ty = lax.axis_index("ty")
    core = lax.rem(tx, CORES)
    pos = tx // CORES
    partner = tx + 1 - 2 * core

    def target(d):
        return lax.rem(pos + 1 + d * (nx - 2), nx) * CORES + core

    def source(d):
        return lax.rem(pos + nx - 1 - d * (nx - 2), nx) * CORES + core

    def owner_rows(d, step):
        o = lax.rem(pos + (nx - 1 - step if d == 0 else 1 + step), nx)
        return pl.ds(pl.multiple_of(o * ob, ob), ob)

    def gather_rows(d, hops):
        o = lax.rem(pos + (nx - hops if d == 0 else hops), nx)
        return pl.ds(pl.multiple_of(o * ob, ob), ob)

    def block_rows(p):
        return pl.ds(pl.multiple_of(lax.rem(ty + 1 + p, ny) * bt, bt), bt)

    barrier = pltpu.get_barrier_semaphore()
    peers = [{"tx": partner}, {"tx": target(0)}, {"tx": target(1)}] + [{"ty": lax.rem(ty + k, ny)} for k in range(1, ny)]
    for peer in peers:
        pl.semaphore_signal(barrier, inc=1, device_id=peer, device_id_type=MESH)

    def w_copies(q, d):
        slot = lax.rem(q, 2)
        j = lax.rem(q, chunks)
        own = pl.ds(pl.multiple_of(core * half + d * dircols + j * width, width), width)
        par = pl.ds(pl.multiple_of(d * dircols + j * width, width), width)
        top, low = pl.ds(0, feats), pl.ds(feats, feats)
        left, right = pl.ds(0, width), pl.ds(width, width)
        dst = wbuf.at[slot, d]
        sem = w_sem.at[slot, d]
        return (pltpu.make_async_copy(wg.at[:, own], dst.at[top, left], sem.at[0]),
                pltpu.make_async_copy(wu.at[:, own], dst.at[top, right], sem.at[1]),
                pltpu.make_async_copy(wgp.at[:, par], dst.at[low, left], sem.at[2]),
                pltpu.make_async_copy(wup.at[:, par], dst.at[low, right], sem.at[3]))

    def w2_copies(q, d, mlp):
        slot = lax.rem(q, 2)
        j = lax.rem(q, chunks)
        dst = w2buf.at[slot]
        rows = pl.ds(d * width, width)
        sem = w2_sem.at[slot, d]
        if mlp:
            mine, theirs, size, first = wd, wdp, half, d * dircols + j * width
        else:
            mine, theirs, size, first = wo, wop, ahalf, d * adir + (j - mlp_chunks) * width
        own = pl.ds(pl.multiple_of(core * size + first, width), width)
        par = pl.ds(pl.multiple_of(first, width), width)
        return (pltpu.make_async_copy(mine.at[own, :], dst.at[0, rows, :], sem.at[0]),
                pltpu.make_async_copy(theirs.at[par, :], dst.at[1, rows, :], sem.at[1]))

    def w2_each(q, action):
        @pl.when(is_mlp(q))
        def _():
            for d in range(2):
                action(w2_copies(q, d, True))

        @pl.when(jnp.logical_not(is_mlp(q)))
        def _():
            for d in range(2):
                action(w2_copies(q, d, False))

    def start(copies):
        for copy in copies:
            copy.start()

    def wait(copies):
        for copy in copies:
            copy.wait()

    def hop(k, d, t):
        slot = lax.rem(t, SLOTS)
        if k < last_hop:
            src, dst = sbuf.at[d, k, slot], rbuf.at[d, k, slot]
        else:
            hslot = lax.rem(t - k + HSLOTS, HSLOTS)
            rows = gather_rows(d, k - last_hop)
            src = dst = hid.at[d, hslot, rows, :]
        return pltpu.make_async_remote_copy(src_ref=src, dst_ref=dst, send_sem=send_sem.at[d, k, slot],
                                            recv_sem=recv_sem.at[d, k, slot], device_id={"tx": target(d)}, device_id_type=MESH)

    def arrival(k, d, t):
        slot = lax.rem(t - 1 + SLOTS, SLOTS)
        if k < last_hop:
            dst = rbuf.at[d, k, slot]
        else:
            hslot = lax.rem(t - 1 - k + HSLOTS, HSLOTS)
            dst = hid.at[d, hslot, gather_rows(d, k - last_hop + 1), :]
        pltpu.make_async_remote_copy(src_ref=dst, dst_ref=dst, send_sem=send_sem.at[d, k, slot], recv_sem=recv_sem.at[d, k, slot],
                                     device_id={"tx": target(d)}, device_id_type=MESH).wait_recv()

    def valid(q):
        return jnp.logical_and(q >= 0, q < total)

    def is_mlp(q):
        return lax.rem(q, chunks) < mlp_chunks

    def reduces(q):
        return jnp.logical_and(valid(q), is_mlp(q))

    def n_copies(p):
        rows = block_rows(p)
        return (pltpu.make_async_copy(nown_hbm.at[rows, :], nown.at[rows, :], n_sem.at[0, p]),
                pltpu.make_async_copy(npar_hbm.at[rows, :], npar.at[rows, :], n_sem.at[1, p]))

    start(n_copies(0))
    for d in range(2):
        start(w_copies(0, d))
    for p in range(1, ny):
        start(n_copies(p))
    loads = (pltpu.make_async_copy(q_hbm, qst, in_sem.at[0]), pltpu.make_async_copy(kv_hbm, kv, in_sem.at[1]))
    start(loads)
    pl.semaphore_wait(barrier, len(peers))
    swaps = []
    for i, (src, dst, size) in enumerate(((wd, wdp, half), (wo, wop, ahalf))):
        rows = pl.ds(pl.multiple_of((1 - core) * size, width), size)
        swaps.append(pltpu.make_async_remote_copy(src_ref=src.at[rows, :], dst_ref=dst, send_sem=gs_sem.at[i], recv_sem=gr_sem.at[i],
                                                  device_id={"tx": partner}, device_id_type=MESH))
    start(swaps)
    wait(loads)

    def attention(p):
        block = lax.rem(ty + 1 + p, ny)
        first = block * bt
        key0 = pl.multiple_of(first // seq_len * seq_len, seq_len)
        keys = kv[0, pl.ds(key0, seq_len), :]
        vals = kv[1, pl.ds(key0, seq_len), :]
        group = 4
        shape = (group * ob, seq_len)
        gap = (first + pos * ob + lax.rem(lax.broadcasted_iota(jnp.int32, shape, 0), ob)
               - key0 - lax.broadcasted_iota(jnp.int32, shape, 1))
        allowed = jnp.logical_and(gap >= 0, gap < WINDOW)
        for g in range(ahalf // HEAD // group):
            cols = [slice((g * group + h) * HEAD, (g * group + h + 1) * HEAD) for h in range(group)]
            queries = jnp.concatenate([qst[block, :, c] for c in cols], axis=0)
            scores = lax.dot_general(queries, keys, (((1,), (1,)), ((), ())), preferred_element_type=F32) * HEAD ** -0.5
            scores = jnp.where(allowed, scores, -1e30)
            weights = jnp.exp(scores - jnp.max(scores, axis=1, keepdims=True))
            norm = jnp.sum(weights, axis=1, keepdims=True)
            mixed = jnp.dot(weights.astype(BF16), vals, preferred_element_type=F32) / norm
            for h, c in enumerate(cols):
                abuf[:, c] = mixed[h * ob:(h + 1) * ob].astype(BF16)

    sends = total + kinds - 1
    signal_end = sends - SLOTS + 1

    def exchange_copy():
        return pltpu.make_async_remote_copy(src_ref=acc.at[1], dst_ref=xrecv, send_sem=xs_sem, recv_sem=xr_sem,
                                            device_id={"tx": partner}, device_id_type=MESH)

    def y_copy(p):
        return pltpu.make_async_remote_copy(src_ref=ysend.at[p], dst_ref=yrecv.at[p], send_sem=ys_sem.at[p], recv_sem=yr_sem.at[p],
                                            device_id={"ty": lax.rem(ty + 1 + p, ny)}, device_id_type=MESH)

    def tick(t, carry):
        @pl.when(jnp.logical_and(t >= SLOTS, t < sends))
        def _():
            for d in range(2):
                pl.semaphore_wait(credit.at[d], 1)

        for k in range(kinds):
            @pl.when((reduces if k < last_hop else valid)(t - SLOTS - k))
            def _():
                for d in range(2):
                    hop(k, d, t - SLOTS).wait_send()

        @pl.when(reduces(t + 1))
        def _():
            for d in range(2):
                start(w_copies(t + 1, d))

        @pl.when(reduces(t))
        def _():
            for d in range(2):
                wait(w_copies(t, d))

            @pl.when(lax.rem(t, chunks) == 0)
            def _():
                wait(n_copies(t // chunks))

            rows = block_rows(t // chunks)
            slot = lax.rem(t, 2)
            pslot = lax.rem(t, nx)

            @pl.loop(0, 2)
            def _(d):
                pbuf[d, pslot] = (jnp.dot(nown[rows, :], wbuf[slot, d, :feats, :], preferred_element_type=F32)
                                  + jnp.dot(npar[rows, :], wbuf[slot, d, feats:, :], preferred_element_type=F32))
            for d in range(2):
                sbuf[d, 0, lax.rem(t, SLOTS)] = pbuf[d, pslot, owner_rows(d, 0), :].astype(BF16)
                hop(0, d, t).start()

        for k in range(1, last_hop + 1):
            @pl.when(reduces(t - k))
            def _():
                for d in range(2):
                    arrival(k - 1, d, t)
                    part = (pbuf[d, lax.rem(t - k + nx, nx), owner_rows(d, k), :]
                            + rbuf[d, k - 1, lax.rem(t - 1 + SLOTS, SLOTS)].astype(F32))
                    if k < last_hop:
                        sbuf[d, k, lax.rem(t, SLOTS)] = part.astype(BF16)
                    else:
                        gate = part[:, :width].astype(BF16).astype(F32)
                        up = part[:, width:].astype(BF16).astype(F32)
                        hslot = lax.rem(t - k + HSLOTS, HSLOTS)
                        hid[d, hslot, gather_rows(d, 0), :] = (gate * jax.nn.sigmoid(gate) * up).astype(BF16)
                    hop(k, d, t).start()

        for i in range(adir // width):
            q = t - last_hop

            @pl.when(jnp.logical_and(valid(q), lax.rem(q, chunks) == mlp_chunks + i))
            def _():
                for d in range(2):
                    hslot = lax.rem(q + HSLOTS, HSLOTS)
                    hid[d, hslot, gather_rows(d, 0), :] = abuf[:, d * adir + i * width:d * adir + (i + 1) * width]
                    hop(last_hop, d, t).start()

        for k in range(last_hop + 1, kinds):
            @pl.when(valid(t - k))
            def _():
                for d in range(2):
                    arrival(k - 1, d, t)
                    hop(k, d, t).start()

        q = t - kinds

        prev = q - 1

        @pl.when(jnp.logical_and(valid(prev), lax.rem(prev + 1, chunks) == 0))
        def _():
            p = prev // chunks
            copy = exchange_copy()
            copy.wait()

            @pl.when(p < ny - 1)
            def _():
                ysend[p] = (acc[0] + xrecv[...]).astype(BF16)
                pl.semaphore_signal(xcredit, inc=1, device_id={"tx": partner}, device_id_type=MESH)
                y_copy(p).start()

            @pl.when(p == ny - 1)
            def _():
                out = acc[0] + xrecv[...]
                for i in range(ny - 1):
                    y_copy(i).wait_recv()
                    out += yrecv[i].astype(F32)
                acc[0] = out

        @pl.when(valid(q))
        def _():
            p = q // chunks

            @pl.when(lax.rem(q, chunks) == 0)
            def _():
                acc[...] = jnp.zeros_like(acc)

            w2_each(q, wait)
            for d in range(2):
                arrival(kinds - 1, d, t)

            hslot = lax.rem(q, HSLOTS)
            slot = lax.rem(q, 2)

            @pl.loop(0, 2)
            def _(o):
                acc[o] += (jnp.dot(hid[0, hslot], w2buf[slot, o, :width, :], preferred_element_type=F32)
                           + jnp.dot(hid[1, hslot], w2buf[slot, o, width:, :], preferred_element_type=F32))

            @pl.when(lax.rem(q + 1, chunks) == 0)
            def _():
                @pl.when(p > 0)
                def _():
                    pl.semaphore_wait(xcredit, 1)
                exchange_copy().start()

        @pl.when(q + 1 == 0)
        def _():
            for copy in swaps:
                copy.wait_recv()

        @pl.when(valid(q + 1))
        def _():
            w2_each(q + 1, start)

        @pl.when(jnp.logical_and(t < total, lax.rem(t, chunks) == chunks // 2))
        def _():
            attention(t // chunks)

        @pl.when(jnp.logical_and(t >= 1, t < signal_end))
        def _():
            for d in range(2):
                pl.semaphore_signal(credit.at[d], inc=1, device_id={"tx": source(d)}, device_id_type=MESH)
        return carry

    lax.fori_loop(0, total + kinds - 1 + SLOTS, tick, 0)
    for i in range(ny - 1):
        y_copy(i).wait_send()
    for copy in swaps:
        copy.wait_send()
    store = pltpu.make_async_copy(acc.at[0], out_ref, in_sem.at[0])
    store.start()
    store.wait()


def mlp_ring(n_own, n_par, q, kv, wg, wu, wgp, wup, wd, wo, nx, ny, width, seq_len):
    tokens, feats = n_own.shape
    bt = tokens // ny
    ob = bt // nx
    cols = wd.shape[1]
    half = wgp.shape[1]
    ahalf = wo.shape[0] // CORES
    kinds = 2 * (nx - 1)
    any_spec = pl.BlockSpec(memory_space=pl.ANY)
    dma = pltpu.SemaphoreType.DMA
    sds = jax.ShapeDtypeStruct
    return pl.pallas_call(
        functools.partial(mlp_kernel, nx, ny, width, seq_len),
        out_shape=(sds((bt, cols), F32), sds((half, cols), BF16), sds((ahalf, cols), BF16)),
        in_specs=[any_spec] * 10, out_specs=[any_spec] * 3,
        scratch_shapes=[
            pltpu.VMEM((tokens, feats), BF16),
            pltpu.VMEM((tokens, feats), BF16),
            pltpu.VMEM((2, 2, 2 * feats, 2 * width), BF16),
            pltpu.VMEM((2, 2, 2 * width, cols), BF16),
            pltpu.VMEM((2, nx, bt, 2 * width), F32),
            pltpu.VMEM((2, nx - 1, SLOTS, ob, 2 * width), BF16),
            pltpu.VMEM((2, nx - 1, SLOTS, ob, 2 * width), BF16),
            pltpu.VMEM((2, HSLOTS, bt, width), BF16),
            pltpu.VMEM((2, bt, cols), F32),
            pltpu.VMEM((bt, cols), F32),
            pltpu.VMEM((ny - 1, bt, cols), BF16),
            pltpu.VMEM((ny - 1, bt, cols), BF16),
            pltpu.VMEM(q.shape, BF16), pltpu.VMEM(kv.shape, BF16), pltpu.VMEM((ob, ahalf), BF16),
            dma((2,)), dma((2, ny)), dma((2, 2, 4)), dma((2, 2, 2)),
            dma((2, kinds, SLOTS)), dma((2, kinds, SLOTS)),
            dma, dma, dma((ny - 1,)), dma((ny - 1,)), dma((2,)), dma((2,)),
            pltpu.SemaphoreType.REGULAR((2,)), pltpu.SemaphoreType.REGULAR,
        ],
        compiler_params=pltpu.CompilerParams(collective_id=1, has_side_effects=True, vmem_limit_bytes=67043328),
        cost_estimate=pl.CostEstimate(flops=400_000_000_000, bytes_accessed=200_000_000, transcendentals=0),
    )(n_own, n_par, q, kv, wg, wu, wgp, wup, wd, wo)


def solution(mesh):
    tx_size = mesh.shape["tx"]
    ty_size = mesh.shape["ty"]
    nx = tx_size // CORES

    def per_device(x_blk, positions, norm_gain, w_q, w_k, w_v, w_o, w_gate, w_up, w_down):
        d_model = x_blk.shape[1] * tx_size
        seq_len = positions.shape[1]
        inv_freq = ROPE_THETA ** (-2.0 * (jnp.arange(HEAD) // 2).astype(F32) / HEAD)
        angle = positions.reshape(-1).astype(F32)[:, None] * inv_freq[None, :]
        cos = jnp.cos(angle)
        sin = jnp.sin(angle) * jnp.where(jnp.arange(HEAD) % 2 == 0, -1.0, 1.0).astype(F32)
        x_wide = x_blk.astype(F32)
        tok_stats = lax.psum(jnp.stack([jnp.sum(x_wide, axis=1), jnp.sum(x_wide * x_wide, axis=1)], axis=1), "tx")
        tok_mean = tok_stats[:, :1] / d_model
        tok_var = tok_stats[:, 1:] / d_model - tok_mean * tok_mean
        normed = (norm_gain * (x_wide - tok_mean) * lax.rsqrt(tok_var + 1e-5)).astype(BF16)
        n_own, n_par, q, kv, wgp, wup = qkv_ring(normed, cos, sin, w_q, w_k, w_v, w_gate, w_up, nx, ty_size)
        block_sum, _, _ = mlp_ring(n_own, n_par, q, kv, w_gate, w_up, wgp, wup, w_down, w_o, nx, ty_size, 256, seq_len)
        return (x_wide + block_sum).astype(BF16)

    in_specs = (P(("dp", "ty"), "tx"), P("dp", None), P("tx"), P("tx", "ty"), P("tx", "ty"), P("tx", "ty"),
                P("ty", "tx"), P("tx", "ty"), P("tx", "ty"), P("ty", "tx"))
    return jax.shard_map(per_device, mesh=mesh, in_specs=in_specs, out_specs=P(("dp", "ty"), "tx"), check_vma=False)
```

```python
import functools
import jax
import jax.numpy as jnp
from jax import lax
from jax.experimental import pallas as pl
from jax.experimental.pallas import tpu as pltpu
from jax.sharding import PartitionSpec as P

HEAD = 128
WINDOW = 4096
ROPE_THETA = 50000
CORES = 2
MESH = pl.DeviceIdType.MESH
F32 = jnp.float32
BF16 = jnp.bfloat16


def swap_lanes(x):
    width = x.shape[1]
    even = lax.rem(lax.broadcasted_iota(jnp.int32, x.shape, 1), 2) == 0
    return jnp.where(even, pltpu.roll(x, width - 1, 1), pltpu.roll(x, 1, 1))


def qkv_kernel(nx, ny, x_ref, gain_ref, cos_ref, sin_ref, wq, wk, wv, wg, wu, nown_out, npar_out, q_out, kv_out, wgp, wup,
               nown, npar, wbuf, pbuf, sbuf, rbuf, qst, kv, stats, st_sem, sr_sem, in_sem, w_sem, ws_sem, wr_sem, ns_sem, nr_sem, ps_sem, pr_sem,
               send_sem, recv_sem, ks_sem, kr_sem, gs_sem, gr_sem):
    tokens, feats = nown.shape
    bt = tokens // ny
    hb = bt // 2
    ob = bt // nx
    half = wgp.shape[1]
    qcols = wq.shape[1] // CORES // 2
    hops = nx - 1
    order = (0, 1, 3, 2)
    tx = lax.axis_index("tx")
    ty = lax.axis_index("ty")
    core = lax.rem(tx, CORES)
    pos = tx // CORES
    partner = tx + 1 - 2 * core
    north, south = lax.rem(ty + 1, ny), lax.rem(ty + ny - 1, ny)

    def chip(i):
        return lax.rem(pos + i, nx) * CORES + core

    def owner_rows(d, step):
        o = lax.rem(pos + (nx - 1 - step if d == 0 else 1 + step), nx)
        return pl.ds(pl.multiple_of(o * ob, ob), ob)

    def rows_of(off):
        return pl.ds(pl.multiple_of(lax.rem(ty + off, ny) * bt, bt), bt)

    def half_rows(off, i):
        return pl.ds(pl.multiple_of(lax.rem(ty + off, ny) * bt + i * hb, hb), hb)

    def remote(src, dst, send, recv, device):
        return pltpu.make_async_remote_copy(src_ref=src, dst_ref=dst, send_sem=send, recv_sem=recv, device_id=device, device_id_type=MESH)

    barrier = pltpu.get_barrier_semaphore()
    group = nx * CORES
    peers = [{"tx": lax.rem(tx + i, group)} for i in range(1, group)] + [{"ty": lax.rem(ty + k, ny)} for k in range(1, ny)]
    for peer in peers:
        pl.semaphore_signal(barrier, inc=1, device_id=peer, device_id_type=MESH)

    def w_parts(c):
        parts = []
        for d in range(2):
            col = pl.ds(pl.multiple_of(c * 2 * qcols + d * qcols, 128), qcols)
            small = pl.ds(pl.multiple_of(c * HEAD, HEAD), HEAD)
            parts.append((wq.at[:, col], d, pl.ds(0, qcols)))
            parts.append(((wk if d == 0 else wv).at[:, small], d, pl.ds(qcols, HEAD)))
        return parts

    local_w = [pltpu.make_async_copy(s, wbuf.at[d, pl.ds(0, feats), cols], w_sem.at[i]) for i, (s, d, cols) in enumerate(w_parts(core))]
    for copy in local_w:
        copy.start()

    x_wide = x_ref[...].astype(F32)
    part_mean = jnp.sum(x_wide, axis=1, keepdims=True) / feats
    centred = x_wide - part_mean
    lane = lax.broadcasted_iota(jnp.int32, (bt, HEAD), 1)
    stats[tx] = jnp.where(lane == 0, part_mean, jnp.sum(centred * centred, axis=1, keepdims=True)).T[:8]

    def stat_copy(i):
        return remote(stats.at[tx], stats.at[tx], st_sem.at[i - 1], sr_sem.at[i - 1], {"tx": lax.rem(tx + i, group)})

    def stat_arrival(i):
        slot = stats.at[lax.rem(tx + group - i, group)]
        return remote(slot, slot, st_sem.at[i - 1], sr_sem.at[i - 1], {"tx": lax.rem(tx + i, group)})

    pl.semaphore_wait(barrier, len(peers))
    for i in range(1, group):
        stat_copy(i).start()
    own = nown.at[rows_of(0), :]
    swap_w = [remote(s, wbuf.at[d, pl.ds(feats, feats), cols], ws_sem.at[i], wr_sem.at[i], {"tx": partner})
              for i, (s, d, cols) in enumerate(w_parts(1 - core))]
    for copy in swap_w:
        copy.start()
    for i in range(1, group):
        stat_arrival(i).wait_recv()
    means = [stats[i, 0:1, :] for i in range(group)]
    mean = sum(means) / group
    var = sum(stats[i, 1:2, :] + feats * (means[i] - mean) * (means[i] - mean) for i in range(group)) / (feats * group)
    sub = lax.broadcasted_iota(jnp.int32, (HEAD, bt), 0)
    cols = jnp.where(sub == 0, mean, lax.rsqrt(var + 1e-5)).T
    nown[rows_of(0), :] = (gain_ref[...] * (x_wide - cols[:, 0:1]) * cols[:, 1:2]).astype(BF16)
    to_south = remote(own, own, ns_sem.at[0], nr_sem.at[0], {"ty": south})
    to_north = remote(own, own, ns_sem.at[1], nr_sem.at[1], {"ty": north})
    to_south.start()
    to_north.start()

    def pair(p):
        rows = rows_of(order[p])
        return remote(nown.at[rows, :], npar.at[rows, :], ps_sem.at[p], pr_sem.at[p], {"tx": partner})

    def far(i):
        rows = half_rows(1 if i == 0 else ny - 1, i)
        return remote(nown.at[rows, :], nown.at[rows, :], ns_sem.at[2 + i], nr_sem.at[2 + i], {"ty": south if i == 0 else north})

    def far_arrival(i):
        rows = half_rows(2, i)
        return remote(nown.at[rows, :], nown.at[rows, :], ns_sem.at[2 + i], nr_sem.at[2 + i], {"ty": south if i == 0 else north})

    def near_arrival(i):
        rows = rows_of(1 if i == 0 else ny - 1)
        return remote(nown.at[rows, :], nown.at[rows, :], ns_sem.at[i], nr_sem.at[i], {"ty": south if i == 0 else north})

    pair(0).start()

    piece = feats // ny
    goff = pl.multiple_of((1 - core) * half, 128)

    def swap_mlp(i):
        rows = pl.ds(i * piece, piece)
        return [remote(src.at[rows, pl.ds(goff, half)], dst.at[rows, :], gs_sem.at[k, i], gr_sem.at[k, i], {"tx": partner})
                for k, (src, dst) in enumerate(((wg, wgp), (wu, wup)))]

    def hop(k, d, p):
        target = chip(1 if d == 0 else nx - 1)
        return remote(sbuf.at[d, k, p], rbuf.at[d, k, p], send_sem.at[d, k, p], recv_sem.at[d, k, p], {"tx": target})

    def kv_rows(p):
        return pl.ds(pl.multiple_of(lax.rem(ty + order[p], ny) * bt + pos * ob, ob), ob)

    def kv_copy(d, p, i):
        rows = kv_rows(p)
        return remote(kv.at[d, rows, :], kv.at[d, rows, :], ks_sem.at[d, p, i - 1], kr_sem.at[d, p, i - 1], {"tx": chip(i)})

    def kv_arrival(d, p, i):
        rows = pl.ds(pl.multiple_of(lax.rem(ty + order[p], ny) * bt + lax.rem(pos + nx - i, nx) * ob, ob), ob)
        return remote(kv.at[d, rows, :], kv.at[d, rows, :], ks_sem.at[d, p, i - 1], kr_sem.at[d, p, i - 1], {"tx": chip(i)})

    def n_store(p):
        rows = rows_of(order[p])
        return (pltpu.make_async_copy(nown.at[rows, :], nown_out.at[rows, :], in_sem.at[1 + 2 * p]),
                pltpu.make_async_copy(npar.at[rows, :], npar_out.at[rows, :], in_sem.at[2 + 2 * p]))

    def product(p):
        pair(p).wait_recv()
        for copy in n_store(p):
            copy.start()
        rows = rows_of(order[p])

        @pl.loop(0, 2)
        def _(d):
            pbuf[d, p] = (jnp.dot(nown[rows, :], wbuf[d, :feats, :], preferred_element_type=F32)
                          + jnp.dot(npar[rows, :], wbuf[d, feats:, :], preferred_element_type=F32))
        for d in range(2):
            sbuf[d, 0, p] = pbuf[d, p, owner_rows(d, 0), :].astype(BF16)
            hop(0, d, p).start()

    def reduce(k, p):
        for d in range(2):
            hop(k - 1, d, p).wait_recv()
            part = pbuf[d, p, owner_rows(d, k), :] + rbuf[d, k - 1, p].astype(F32)
            if k < hops:
                sbuf[d, k, p] = part.astype(BF16)
                hop(k, d, p).start()
                continue
            rows = kv_rows(p)
            block = lax.rem(ty + order[p], ny)
            part = part.astype(BF16).astype(F32)
            cos, sin = cos_ref[block], sin_ref[block]
            small = part[:, qcols:]
            if d == 0:
                small = small * cos + swap_lanes(small) * sin
            kv[d, rows, :] = small.astype(BF16)
            for i in range(1, nx):
                kv_copy(d, p, i).start()
            for h in range(qcols // HEAD):
                head = part[:, h * HEAD:(h + 1) * HEAD]
                qst[block, :, d * qcols + h * HEAD:d * qcols + (h + 1) * HEAD] = (head * cos + swap_lanes(head) * sin).astype(BF16)

    def give(i):
        for copy in swap_mlp(i):
            copy.start()

    for copy in local_w:
        copy.wait()
    for copy in swap_w:
        copy.wait_recv()
    product(0)
    give(0)
    give(1)
    reduce(1, 0)
    give(2)
    reduce(2, 0)
    near_arrival(0).wait_recv()
    far(0).start()
    pair(1).start()
    near_arrival(1).wait_recv()
    far(1).start()
    pair(2).start()
    reduce(3, 0)
    product(1)
    product(2)
    reduce(1, 1)
    reduce(1, 2)
    far_arrival(0).wait_recv()
    far_arrival(1).wait_recv()
    pair(3).start()
    reduce(2, 1)
    reduce(2, 2)
    product(3)
    give(3)
    reduce(3, 1)
    reduce(3, 2)
    reduce(1, 3)
    reduce(2, 3)
    reduce(3, 3)

    for p in range(ny):
        for d in range(2):
            for i in range(1, nx):
                kv_arrival(d, p, i).wait_recv()
                kv_copy(d, p, i).wait_send()
            for k in range(hops):
                hop(k, d, p).wait_send()
        pair(p).wait_send()
        for copy in n_store(p):
            copy.wait()
        for copy in swap_mlp(p):
            copy.wait()
    for copy in swap_w:
        copy.wait_send()
    for i in range(1, group):
        stat_copy(i).wait_send()
    to_south.wait_send()
    to_north.wait_send()
    far(0).wait_send()
    far(1).wait_send()
    stores = (pltpu.make_async_copy(qst, q_out, in_sem.at[0]), pltpu.make_async_copy(kv, kv_out, in_sem.at[1]))
    for copy in stores:
        copy.start()
    for copy in stores:
        copy.wait()


def qkv_ring(x_blk, gain, cos, sin, wq, wk, wv, wg, wu, nx, ny):
    bt, feats = x_blk.shape
    tokens = bt * ny
    ob = bt // nx
    half = wg.shape[1] // CORES
    qhalf = wq.shape[1] // CORES
    cols = qhalf // 2 + HEAD
    hops = nx - 1
    any_spec = pl.BlockSpec(memory_space=pl.ANY)
    vmem = pl.BlockSpec(memory_space=pltpu.VMEM)
    dma = pltpu.SemaphoreType.DMA
    sds = jax.ShapeDtypeStruct
    return pl.pallas_call(
        functools.partial(qkv_kernel, nx, ny),
        out_shape=(sds((tokens, feats), BF16), sds((tokens, feats), BF16), sds((ny, ob, qhalf), BF16), sds((2, tokens, HEAD), BF16),
                   sds((feats, half), BF16), sds((feats, half), BF16)),
        in_specs=[vmem] * 4 + [any_spec] * 5, out_specs=[any_spec] * 6,
        scratch_shapes=[
            pltpu.VMEM((tokens, feats), BF16), pltpu.VMEM((tokens, feats), BF16),
            pltpu.VMEM((2, 2 * feats, cols), BF16),
            pltpu.VMEM((2, nx, bt, cols), F32),
            pltpu.VMEM((2, hops, ny, ob, cols), BF16), pltpu.VMEM((2, hops, ny, ob, cols), BF16),
            pltpu.VMEM((ny, ob, qhalf), BF16), pltpu.VMEM((2, tokens, HEAD), BF16),
            pltpu.VMEM((nx * CORES, 8, bt), F32), dma((nx * CORES - 1,)), dma((nx * CORES - 1,)),
            dma((1 + 2 * ny,)), dma((4,)), dma((4,)), dma((4,)), dma((4,)), dma((4,)), dma((ny,)), dma((ny,)),
            dma((2, hops, ny)), dma((2, hops, ny)), dma((2, ny, hops)), dma((2, ny, hops)), dma((2, ny)), dma((2, ny)),
        ],
        compiler_params=pltpu.CompilerParams(collective_id=0, has_side_effects=True, vmem_limit_bytes=60 << 20),
        cost_estimate=pl.CostEstimate(flops=60_000_000_000, bytes_accessed=60_000_000, transcendentals=0),
    )(x_blk, gain, cos, sin, wq, wk, wv, wg, wu)


SLOTS = 3
HSLOTS = 8


def mlp_kernel(nx, ny, width, seq_len, nown_hbm, npar_hbm, q_hbm, kv_hbm, wg, wu, wgp, wup, wd, wo, out_ref, wdp, wop,
               nown, npar, wbuf, w2buf, pbuf, sbuf, rbuf, hid, acc, xrecv, ysend, yrecv, qst, kv, abuf,
               in_sem, n_sem, w_sem, w2_sem, send_sem, recv_sem, xs_sem, xr_sem, ys_sem, yr_sem, gs_sem, gr_sem, credit, xcredit):
    tokens, feats = nown.shape
    bt = tokens // ny
    ob = bt // nx
    half = wgp.shape[1]
    dircols = half // 2
    ahalf = wop.shape[0]
    adir = ahalf // 2
    mlp_chunks = dircols // width
    chunks = mlp_chunks + adir // width
    total = ny * chunks
    last_hop = nx - 1
    kinds = 2 * last_hop
    tx = lax.axis_index("tx")
    ty = lax.axis_index("ty")
    core = lax.rem(tx, CORES)
    pos = tx // CORES
    partner = tx + 1 - 2 * core

    def target(d):
        return lax.rem(pos + 1 + d * (nx - 2), nx) * CORES + core

    def source(d):
        return lax.rem(pos + nx - 1 - d * (nx - 2), nx) * CORES + core

    def owner_rows(d, step):
        o = lax.rem(pos + (nx - 1 - step if d == 0 else 1 + step), nx)
        return pl.ds(pl.multiple_of(o * ob, ob), ob)

    def gather_rows(d, hops):
        o = lax.rem(pos + (nx - hops if d == 0 else hops), nx)
        return pl.ds(pl.multiple_of(o * ob, ob), ob)

    def block_rows(p):
        return pl.ds(pl.multiple_of(lax.rem(ty + 1 + p, ny) * bt, bt), bt)

    barrier = pltpu.get_barrier_semaphore()
    peers = [{"tx": partner}, {"tx": target(0)}, {"tx": target(1)}] + [{"ty": lax.rem(ty + k, ny)} for k in range(1, ny)]
    for peer in peers:
        pl.semaphore_signal(barrier, inc=1, device_id=peer, device_id_type=MESH)

    def w_copies(q, d):
        slot = lax.rem(q, 2)
        j = lax.rem(q, chunks)
        own = pl.ds(pl.multiple_of(core * half + d * dircols + j * width, width), width)
        par = pl.ds(pl.multiple_of(d * dircols + j * width, width), width)
        top, low = pl.ds(0, feats), pl.ds(feats, feats)
        left, right = pl.ds(0, width), pl.ds(width, width)
        dst = wbuf.at[slot, d]
        sem = w_sem.at[slot, d]
        return (pltpu.make_async_copy(wg.at[:, own], dst.at[top, left], sem.at[0]),
                pltpu.make_async_copy(wu.at[:, own], dst.at[top, right], sem.at[1]),
                pltpu.make_async_copy(wgp.at[:, par], dst.at[low, left], sem.at[2]),
                pltpu.make_async_copy(wup.at[:, par], dst.at[low, right], sem.at[3]))

    def w2_copies(q, d, mlp):
        slot = lax.rem(q, 2)
        j = lax.rem(q, chunks)
        dst = w2buf.at[slot]
        rows = pl.ds(d * width, width)
        sem = w2_sem.at[slot, d]
        if mlp:
            mine, theirs, size, first = wd, wdp, half, d * dircols + j * width
        else:
            mine, theirs, size, first = wo, wop, ahalf, d * adir + (j - mlp_chunks) * width
        own = pl.ds(pl.multiple_of(core * size + first, width), width)
        par = pl.ds(pl.multiple_of(first, width), width)
        return (pltpu.make_async_copy(mine.at[own, :], dst.at[0, rows, :], sem.at[0]),
                pltpu.make_async_copy(theirs.at[par, :], dst.at[1, rows, :], sem.at[1]))

    def w2_each(q, action):
        @pl.when(is_mlp(q))
        def _():
            for d in range(2):
                action(w2_copies(q, d, True))

        @pl.when(jnp.logical_not(is_mlp(q)))
        def _():
            for d in range(2):
                action(w2_copies(q, d, False))

    def start(copies):
        for copy in copies:
            copy.start()

    def wait(copies):
        for copy in copies:
            copy.wait()

    def hop(k, d, t):
        slot = lax.rem(t, SLOTS)
        if k < last_hop:
            src, dst = sbuf.at[d, k, slot], rbuf.at[d, k, slot]
        else:
            hslot = lax.rem(t - k + HSLOTS, HSLOTS)
            rows = gather_rows(d, k - last_hop)
            src = dst = hid.at[d, hslot, rows, :]
        return pltpu.make_async_remote_copy(src_ref=src, dst_ref=dst, send_sem=send_sem.at[d, k, slot],
                                            recv_sem=recv_sem.at[d, k, slot], device_id={"tx": target(d)}, device_id_type=MESH)

    def arrival(k, d, t):
        slot = lax.rem(t - 1 + SLOTS, SLOTS)
        if k < last_hop:
            dst = rbuf.at[d, k, slot]
        else:
            hslot = lax.rem(t - 1 - k + HSLOTS, HSLOTS)
            dst = hid.at[d, hslot, gather_rows(d, k - last_hop + 1), :]
        pltpu.make_async_remote_copy(src_ref=dst, dst_ref=dst, send_sem=send_sem.at[d, k, slot], recv_sem=recv_sem.at[d, k, slot],
                                     device_id={"tx": target(d)}, device_id_type=MESH).wait_recv()

    def valid(q):
        return jnp.logical_and(q >= 0, q < total)

    def is_mlp(q):
        return lax.rem(q, chunks) < mlp_chunks

    def reduces(q):
        return jnp.logical_and(valid(q), is_mlp(q))

    def n_copies(p):
        rows = block_rows(p)
        return (pltpu.make_async_copy(nown_hbm.at[rows, :], nown.at[rows, :], n_sem.at[0, p]),
                pltpu.make_async_copy(npar_hbm.at[rows, :], npar.at[rows, :], n_sem.at[1, p]))

    start(n_copies(0))
    for d in range(2):
        start(w_copies(0, d))
    loads = (pltpu.make_async_copy(q_hbm, qst, in_sem.at[0]), pltpu.make_async_copy(kv_hbm, kv, in_sem.at[1]))
    pl.semaphore_wait(barrier, len(peers))
    swaps = []
    for i, (src, dst, size) in enumerate(((wd, wdp, half), (wo, wop, ahalf))):
        rows = pl.ds(pl.multiple_of((1 - core) * size, width), size)
        swaps.append(pltpu.make_async_remote_copy(src_ref=src.at[rows, :], dst_ref=dst, send_sem=gs_sem.at[i], recv_sem=gr_sem.at[i],
                                                  device_id={"tx": partner}, device_id_type=MESH))

    def attention(p):
        block = lax.rem(ty + 1 + p, ny)
        first = block * bt
        key0 = pl.multiple_of(first // seq_len * seq_len, seq_len)
        keys = kv[0, pl.ds(key0, seq_len), :]
        vals = kv[1, pl.ds(key0, seq_len), :]
        group = 4
        shape = (group * ob, seq_len)
        gap = (first + pos * ob + lax.rem(lax.broadcasted_iota(jnp.int32, shape, 0), ob)
               - key0 - lax.broadcasted_iota(jnp.int32, shape, 1))
        allowed = jnp.logical_and(gap >= 0, gap < WINDOW)
        for g in range(ahalf // HEAD // group):
            cols = [slice((g * group + h) * HEAD, (g * group + h + 1) * HEAD) for h in range(group)]
            queries = jnp.concatenate([qst[block, :, c] for c in cols], axis=0)
            scores = lax.dot_general(queries, keys, (((1,), (1,)), ((), ())), preferred_element_type=F32) * HEAD ** -0.5
            scores = jnp.where(allowed, scores, -1e30)
            weights = jnp.exp(scores - jnp.max(scores, axis=1, keepdims=True))
            norm = jnp.sum(weights, axis=1, keepdims=True)
            mixed = jnp.dot(weights.astype(BF16), vals, preferred_element_type=F32) / norm
            for h, c in enumerate(cols):
                abuf[:, c] = mixed[h * ob:(h + 1) * ob].astype(BF16)

    sends = total + kinds - 1
    signal_end = sends - SLOTS + 1

    def exchange_copy():
        return pltpu.make_async_remote_copy(src_ref=acc.at[1], dst_ref=xrecv, send_sem=xs_sem, recv_sem=xr_sem,
                                            device_id={"tx": partner}, device_id_type=MESH)

    def y_copy(p):
        return pltpu.make_async_remote_copy(src_ref=ysend.at[p], dst_ref=yrecv.at[p], send_sem=ys_sem.at[p], recv_sem=yr_sem.at[p],
                                            device_id={"ty": lax.rem(ty + 1 + p, ny)}, device_id_type=MESH)

    def tick(t, carry):
        @pl.when(jnp.logical_and(t >= SLOTS, t < sends))
        def _():
            for d in range(2):
                pl.semaphore_wait(credit.at[d], 1)

        for k in range(kinds):
            @pl.when((reduces if k < last_hop else valid)(t - SLOTS - k))
            def _():
                for d in range(2):
                    hop(k, d, t - SLOTS).wait_send()

        @pl.when(reduces(t + 1))
        def _():
            for d in range(2):
                start(w_copies(t + 1, d))

        @pl.when(reduces(t))
        def _():
            for d in range(2):
                wait(w_copies(t, d))

            @pl.when(lax.rem(t, chunks) == 0)
            def _():
                wait(n_copies(t // chunks))

            rows = block_rows(t // chunks)
            slot = lax.rem(t, 2)
            pslot = lax.rem(t, nx)

            @pl.loop(0, 2)
            def _(d):
                pbuf[d, pslot] = (jnp.dot(nown[rows, :], wbuf[slot, d, :feats, :], preferred_element_type=F32)
                                  + jnp.dot(npar[rows, :], wbuf[slot, d, feats:, :], preferred_element_type=F32))
            for d in range(2):
                sbuf[d, 0, lax.rem(t, SLOTS)] = pbuf[d, pslot, owner_rows(d, 0), :].astype(BF16)
                hop(0, d, t).start()

        @pl.when(t == 1)
        def _():
            start(swaps)
            start(loads)
            for p in range(1, ny):
                start(n_copies(p))

        for k in range(1, last_hop + 1):
            @pl.when(reduces(t - k))
            def _():
                for d in range(2):
                    arrival(k - 1, d, t)
                    part = (pbuf[d, lax.rem(t - k + nx, nx), owner_rows(d, k), :]
                            + rbuf[d, k - 1, lax.rem(t - 1 + SLOTS, SLOTS)].astype(F32))
                    if k < last_hop:
                        sbuf[d, k, lax.rem(t, SLOTS)] = part.astype(BF16)
                    else:
                        gate = part[:, :width].astype(BF16).astype(F32)
                        up = part[:, width:].astype(BF16).astype(F32)
                        hslot = lax.rem(t - k + HSLOTS, HSLOTS)
                        hid[d, hslot, gather_rows(d, 0), :] = (gate * jax.nn.sigmoid(gate) * up).astype(BF16)
                    hop(k, d, t).start()

        for i in range(adir // width):
            q = t - last_hop

            @pl.when(jnp.logical_and(valid(q), lax.rem(q, chunks) == mlp_chunks + i))
            def _():
                for d in range(2):
                    hslot = lax.rem(q + HSLOTS, HSLOTS)
                    hid[d, hslot, gather_rows(d, 0), :] = abuf[:, d * adir + i * width:d * adir + (i + 1) * width]
                    hop(last_hop, d, t).start()

        for k in range(last_hop + 1, kinds):
            @pl.when(valid(t - k))
            def _():
                for d in range(2):
                    arrival(k - 1, d, t)
                    hop(k, d, t).start()

        q = t - kinds

        prev = q - 1

        @pl.when(jnp.logical_and(valid(prev), lax.rem(prev + 1, chunks) == 0))
        def _():
            p = prev // chunks
            copy = exchange_copy()
            copy.wait()

            @pl.when(p < ny - 1)
            def _():
                ysend[p] = (acc[0] + xrecv[...]).astype(BF16)
                pl.semaphore_signal(xcredit, inc=1, device_id={"tx": partner}, device_id_type=MESH)
                y_copy(p).start()

            @pl.when(p == ny - 1)
            def _():
                out = acc[0] + xrecv[...]
                for i in range(ny - 1):
                    y_copy(i).wait_recv()
                    out += yrecv[i].astype(F32)
                acc[0] = out

        @pl.when(valid(q))
        def _():
            p = q // chunks

            @pl.when(lax.rem(q, chunks) == 0)
            def _():
                acc[...] = jnp.zeros_like(acc)

            w2_each(q, wait)
            for d in range(2):
                arrival(kinds - 1, d, t)

            hslot = lax.rem(q, HSLOTS)
            slot = lax.rem(q, 2)

            @pl.loop(0, 2)
            def _(o):
                acc[o] += (jnp.dot(hid[0, hslot], w2buf[slot, o, :width, :], preferred_element_type=F32)
                           + jnp.dot(hid[1, hslot], w2buf[slot, o, width:, :], preferred_element_type=F32))

            @pl.when(lax.rem(q + 1, chunks) == 0)
            def _():
                @pl.when(p > 0)
                def _():
                    pl.semaphore_wait(xcredit, 1)
                exchange_copy().start()

        @pl.when(q + 1 == 0)
        def _():
            for copy in swaps:
                copy.wait_recv()

        @pl.when(valid(q + 1))
        def _():
            w2_each(q + 1, start)

        @pl.when(jnp.logical_and(t < total, lax.rem(t, chunks) == chunks // 2))
        def _():
            @pl.when(t < chunks)
            def _():
                wait(loads)
            attention(t // chunks)

        @pl.when(jnp.logical_and(t >= 1, t < signal_end))
        def _():
            for d in range(2):
                pl.semaphore_signal(credit.at[d], inc=1, device_id={"tx": source(d)}, device_id_type=MESH)
        return carry

    lax.fori_loop(0, total + kinds - 1 + SLOTS, tick, 0)
    for i in range(ny - 1):
        y_copy(i).wait_send()
    for copy in swaps:
        copy.wait_send()
    store = pltpu.make_async_copy(acc.at[0], out_ref, in_sem.at[0])
    store.start()
    store.wait()


def mlp_ring(n_own, n_par, q, kv, wg, wu, wgp, wup, wd, wo, nx, ny, width, seq_len):
    tokens, feats = n_own.shape
    bt = tokens // ny
    ob = bt // nx
    cols = wd.shape[1]
    half = wgp.shape[1]
    ahalf = wo.shape[0] // CORES
    kinds = 2 * (nx - 1)
    any_spec = pl.BlockSpec(memory_space=pl.ANY)
    dma = pltpu.SemaphoreType.DMA
    sds = jax.ShapeDtypeStruct
    return pl.pallas_call(
        functools.partial(mlp_kernel, nx, ny, width, seq_len),
        out_shape=(sds((bt, cols), F32), sds((half, cols), BF16), sds((ahalf, cols), BF16)),
        in_specs=[any_spec] * 10, out_specs=[any_spec] * 3,
        scratch_shapes=[
            pltpu.VMEM((tokens, feats), BF16),
            pltpu.VMEM((tokens, feats), BF16),
            pltpu.VMEM((2, 2, 2 * feats, 2 * width), BF16),
            pltpu.VMEM((2, 2, 2 * width, cols), BF16),
            pltpu.VMEM((2, nx, bt, 2 * width), F32),
            pltpu.VMEM((2, nx - 1, SLOTS, ob, 2 * width), BF16),
            pltpu.VMEM((2, nx - 1, SLOTS, ob, 2 * width), BF16),
            pltpu.VMEM((2, HSLOTS, bt, width), BF16),
            pltpu.VMEM((2, bt, cols), F32),
            pltpu.VMEM((bt, cols), F32),
            pltpu.VMEM((ny - 1, bt, cols), BF16),
            pltpu.VMEM((ny - 1, bt, cols), BF16),
            pltpu.VMEM(q.shape, BF16), pltpu.VMEM(kv.shape, BF16), pltpu.VMEM((ob, ahalf), BF16),
            dma((2,)), dma((2, ny)), dma((2, 2, 4)), dma((2, 2, 2)),
            dma((2, kinds, SLOTS)), dma((2, kinds, SLOTS)),
            dma, dma, dma((ny - 1,)), dma((ny - 1,)), dma((2,)), dma((2,)),
            pltpu.SemaphoreType.REGULAR((2,)), pltpu.SemaphoreType.REGULAR,
        ],
        compiler_params=pltpu.CompilerParams(collective_id=1, has_side_effects=True, vmem_limit_bytes=67043328),
        cost_estimate=pl.CostEstimate(flops=400_000_000_000, bytes_accessed=200_000_000, transcendentals=0),
    )(n_own, n_par, q, kv, wg, wu, wgp, wup, wd, wo)


def solution(mesh):
    tx_size = mesh.shape["tx"]
    ty_size = mesh.shape["ty"]
    nx = tx_size // CORES

    def per_device(x_blk, positions, norm_gain, w_q, w_k, w_v, w_o, w_gate, w_up, w_down):
        seq_len = positions.shape[1]
        inv_freq = ROPE_THETA ** (-2.0 * (jnp.arange(HEAD) // 2).astype(F32) / HEAD)
        own_pos = positions.reshape(ty_size, nx, -1)
        own_pos = lax.dynamic_index_in_dim(own_pos, lax.axis_index("tx") // CORES, 1, keepdims=False)
        angle = own_pos.astype(F32)[:, :, None] * inv_freq
        cos = jnp.cos(angle)
        sin = jnp.sin(angle) * jnp.where(jnp.arange(HEAD) % 2 == 0, -1.0, 1.0).astype(F32)
        n_own, n_par, q, kv, wgp, wup = qkv_ring(x_blk, norm_gain[None, :], cos, sin, w_q, w_k, w_v, w_gate, w_up, nx, ty_size)
        block_sum, _, _ = mlp_ring(n_own, n_par, q, kv, w_gate, w_up, wgp, wup, w_down, w_o, nx, ty_size, 256, seq_len)
        return (x_blk.astype(F32) + block_sum).astype(BF16)

    in_specs = (P(("dp", "ty"), "tx"), P("dp", None), P("tx"), P("tx", "ty"), P("tx", "ty"), P("tx", "ty"),
                P("ty", "tx"), P("tx", "ty"), P("tx", "ty"), P("ty", "tx"))
    return jax.shard_map(per_device, mesh=mesh, in_specs=in_specs, out_specs=P(("dp", "ty"), "tx"), check_vma=False)
```

```python
import functools
import jax
import jax.numpy as jnp
from jax import lax
from jax.experimental import pallas as pl
from jax.experimental.pallas import tpu as pltpu
from jax.sharding import PartitionSpec as P

HEAD = 128
WINDOW = 4096
ROPE_THETA = 50000
CORES = 2
WIDTH = 256
EARLY = 3
MESH = pl.DeviceIdType.MESH
F32 = jnp.float32
BF16 = jnp.bfloat16


def swap_lanes(x):
    width = x.shape[1]
    even = lax.rem(lax.broadcasted_iota(jnp.int32, x.shape, 1), 2) == 0
    return jnp.where(even, pltpu.roll(x, width - 1, 1), pltpu.roll(x, 1, 1))


def qkv_kernel(nx, ny, x_ref, gain_ref, cos_ref, sin_ref, wq, wk, wv, wg, wu, nown_out, npar_out, q_out, kv_out, wgp, wup, h_out,
               nown, npar, wbuf, pbuf, sbuf, rbuf, qst, kv, wm, pm, sm, rm, hst, wl_sem, wms_sem, wmr_sem, ms_sem, mr_sem, stats, st_sem, sr_sem, in_sem, w_sem, ws_sem, wr_sem, ns_sem, nr_sem, ps_sem, pr_sem,
               send_sem, recv_sem, ks_sem, kr_sem, gs_sem, gr_sem):
    tokens, feats = nown.shape
    bt = tokens // ny
    hb = bt // 2
    ob = bt // nx
    half = wgp.shape[1]
    qcols = wq.shape[1] // CORES // 2
    hops = nx - 1
    order = (0, 1, 3, 2)
    tx = lax.axis_index("tx")
    ty = lax.axis_index("ty")
    core = lax.rem(tx, CORES)
    pos = tx // CORES
    partner = tx + 1 - 2 * core
    north, south = lax.rem(ty + 1, ny), lax.rem(ty + ny - 1, ny)

    def chip(i):
        return lax.rem(pos + i, nx) * CORES + core

    def owner_rows(d, step):
        o = lax.rem(pos + (nx - 1 - step if d == 0 else 1 + step), nx)
        return pl.ds(pl.multiple_of(o * ob, ob), ob)

    def rows_of(off):
        return pl.ds(pl.multiple_of(lax.rem(ty + off, ny) * bt, bt), bt)

    def half_rows(off, i):
        return pl.ds(pl.multiple_of(lax.rem(ty + off, ny) * bt + i * hb, hb), hb)

    def remote(src, dst, send, recv, device):
        return pltpu.make_async_remote_copy(src_ref=src, dst_ref=dst, send_sem=send, recv_sem=recv, device_id=device, device_id_type=MESH)

    barrier = pltpu.get_barrier_semaphore()
    group = nx * CORES
    peers = [{"tx": lax.rem(tx + i, group)} for i in range(1, group)] + [{"ty": lax.rem(ty + k, ny)} for k in range(1, ny)]
    for peer in peers:
        pl.semaphore_signal(barrier, inc=1, device_id=peer, device_id_type=MESH)

    def w_parts(c):
        parts = []
        for d in range(2):
            col = pl.ds(pl.multiple_of(c * 2 * qcols + d * qcols, 128), qcols)
            small = pl.ds(pl.multiple_of(c * HEAD, HEAD), HEAD)
            parts.append((wq.at[:, col], d, pl.ds(0, qcols)))
            parts.append(((wk if d == 0 else wv).at[:, small], d, pl.ds(qcols, HEAD)))
        return parts

    def early_parts(c, m):
        for d in range(2):
            col = pl.ds(pl.multiple_of(c * half + d * (half // 2) + m * WIDTH, WIDTH), WIDTH)
            for i, src in enumerate((wg, wu)):
                yield src.at[:, col], d, i, pl.ds(i * WIDTH, WIDTH)

    local_w = [pltpu.make_async_copy(s, wbuf.at[d, pl.ds(0, feats), cols], w_sem.at[i]) for i, (s, d, cols) in enumerate(w_parts(core))]
    for copy in local_w:
        copy.start()

    x_wide = x_ref[...].astype(F32)
    part_mean = jnp.sum(x_wide, axis=1, keepdims=True) / feats
    centred = x_wide - part_mean
    lane = lax.broadcasted_iota(jnp.int32, (bt, HEAD), 1)
    stats[tx] = jnp.where(lane == 0, part_mean, jnp.sum(centred * centred, axis=1, keepdims=True)).T[:8]

    def stat_copy(i):
        return remote(stats.at[tx], stats.at[tx], st_sem.at[i - 1], sr_sem.at[i - 1], {"tx": lax.rem(tx + i, group)})

    def stat_arrival(i):
        slot = stats.at[lax.rem(tx + group - i, group)]
        return remote(slot, slot, st_sem.at[i - 1], sr_sem.at[i - 1], {"tx": lax.rem(tx + i, group)})

    pl.semaphore_wait(barrier, len(peers))
    for i in range(1, group):
        stat_copy(i).start()
    own = nown.at[rows_of(0), :]
    swap_w = [remote(s, wbuf.at[d, pl.ds(feats, feats), cols], ws_sem.at[i], wr_sem.at[i], {"tx": partner})
              for i, (s, d, cols) in enumerate(w_parts(1 - core))]
    for copy in swap_w:
        copy.start()
    for i in range(1, group):
        stat_arrival(i).wait_recv()
    means = [stats[i, 0:1, :] for i in range(group)]
    mean = sum(means) / group
    var = sum(stats[i, 1:2, :] + feats * (means[i] - mean) * (means[i] - mean) for i in range(group)) / (feats * group)
    sub = lax.broadcasted_iota(jnp.int32, (HEAD, bt), 0)
    cols = jnp.where(sub == 0, mean, lax.rsqrt(var + 1e-5)).T
    nown[rows_of(0), :] = (gain_ref[...] * (x_wide - cols[:, 0:1]) * cols[:, 1:2]).astype(BF16)
    to_south = remote(own, own, ns_sem.at[0], nr_sem.at[0], {"ty": south})
    to_north = remote(own, own, ns_sem.at[1], nr_sem.at[1], {"ty": north})
    to_south.start()
    to_north.start()

    early_local = [[pltpu.make_async_copy(src, wm.at[d, m, pl.ds(0, feats), cols], wl_sem.at[m, d, i])
                    for src, d, i, cols in early_parts(core, m)] for m in range(EARLY)]
    early_swap = [[remote(src, wm.at[d, m, pl.ds(feats, feats), cols], wms_sem.at[m, d, i], wmr_sem.at[m, d, i], {"tx": partner})
                   for src, d, i, cols in early_parts(1 - core, m)] for m in range(EARLY)]

    def pair(p):
        rows = rows_of(order[p])
        return remote(nown.at[rows, :], npar.at[rows, :], ps_sem.at[p], pr_sem.at[p], {"tx": partner})

    def far(i):
        rows = half_rows(1 if i == 0 else ny - 1, i)
        return remote(nown.at[rows, :], nown.at[rows, :], ns_sem.at[2 + i], nr_sem.at[2 + i], {"ty": south if i == 0 else north})

    def far_arrival(i):
        rows = half_rows(2, i)
        return remote(nown.at[rows, :], nown.at[rows, :], ns_sem.at[2 + i], nr_sem.at[2 + i], {"ty": south if i == 0 else north})

    def near_arrival(i):
        rows = rows_of(1 if i == 0 else ny - 1)
        return remote(nown.at[rows, :], nown.at[rows, :], ns_sem.at[i], nr_sem.at[i], {"ty": south if i == 0 else north})

    pair(0).start()
    for m in range(EARLY):
        for copy in early_local[m] + early_swap[m]:
            copy.start()

    piece = feats // ny
    goff = pl.multiple_of((1 - core) * half, 128)

    def swap_mlp(i):
        rows = pl.ds(i * piece, piece)
        return [remote(src.at[rows, pl.ds(goff, half)], dst.at[rows, :], gs_sem.at[k, i], gr_sem.at[k, i], {"tx": partner})
                for k, (src, dst) in enumerate(((wg, wgp), (wu, wup)))]

    def hop(k, d, p):
        target = chip(1 if d == 0 else nx - 1)
        return remote(sbuf.at[d, k, p], rbuf.at[d, k, p], send_sem.at[d, k, p], recv_sem.at[d, k, p], {"tx": target})

    def kv_rows(p):
        return pl.ds(pl.multiple_of(lax.rem(ty + order[p], ny) * bt + pos * ob, ob), ob)

    def kv_copy(d, p, i):
        rows = kv_rows(p)
        return remote(kv.at[d, rows, :], kv.at[d, rows, :], ks_sem.at[d, p, i - 1], kr_sem.at[d, p, i - 1], {"tx": chip(i)})

    def kv_arrival(d, p, i):
        rows = pl.ds(pl.multiple_of(lax.rem(ty + order[p], ny) * bt + lax.rem(pos + nx - i, nx) * ob, ob), ob)
        return remote(kv.at[d, rows, :], kv.at[d, rows, :], ks_sem.at[d, p, i - 1], kr_sem.at[d, p, i - 1], {"tx": chip(i)})

    def n_store(p):
        rows = rows_of(order[p])
        return (pltpu.make_async_copy(nown.at[rows, :], nown_out.at[rows, :], in_sem.at[1 + 2 * p]),
                pltpu.make_async_copy(npar.at[rows, :], npar_out.at[rows, :], in_sem.at[2 + 2 * p]))

    def product(p):
        pair(p).wait_recv()
        for copy in n_store(p):
            copy.start()
        rows = rows_of(order[p])

        @pl.loop(0, 2)
        def _(d):
            pbuf[d, p] = (jnp.dot(nown[rows, :], wbuf[d, :feats, :], preferred_element_type=F32)
                          + jnp.dot(npar[rows, :], wbuf[d, feats:, :], preferred_element_type=F32))
        for d in range(2):
            sbuf[d, 0, p] = pbuf[d, p, owner_rows(d, 0), :].astype(BF16)
            hop(0, d, p).start()

    def reduce(k, p):
        for d in range(2):
            hop(k - 1, d, p).wait_recv()
            part = pbuf[d, p, owner_rows(d, k), :] + rbuf[d, k - 1, p].astype(F32)
            if k < hops:
                sbuf[d, k, p] = part.astype(BF16)
                hop(k, d, p).start()
                continue
            rows = kv_rows(p)
            block = lax.rem(ty + order[p], ny)
            part = part.astype(BF16).astype(F32)
            cos, sin = cos_ref[block], sin_ref[block]
            small = part[:, qcols:]
            if d == 0:
                small = small * cos + swap_lanes(small) * sin
            kv[d, rows, :] = small.astype(BF16)
            for i in range(1, nx):
                kv_copy(d, p, i).start()
            for h in range(qcols // HEAD):
                head = part[:, h * HEAD:(h + 1) * HEAD]
                qst[block, :, d * qcols + h * HEAD:d * qcols + (h + 1) * HEAD] = (head * cos + swap_lanes(head) * sin).astype(BF16)

    def give(i):
        for copy in swap_mlp(i):
            copy.start()

    def early_hop(k, d, m):
        target = chip(1 if d == 0 else nx - 1)
        return remote(sm.at[d, k, m], rm.at[d, k, m], ms_sem.at[d, k, m], mr_sem.at[d, k, m], {"tx": target})

    def early_product(m):
        for copy in early_local[m]:
            copy.wait()
        for copy in early_swap[m]:
            copy.wait_recv()
        rows = rows_of(0)

        @pl.loop(0, 2)
        def _(d):
            pm[d, m] = (jnp.dot(nown[rows, :], wm[d, m, :feats, :], preferred_element_type=F32)
                        + jnp.dot(npar[rows, :], wm[d, m, feats:, :], preferred_element_type=F32))
        for d in range(2):
            sm[d, 0, m] = pm[d, m, owner_rows(d, 0), :].astype(BF16)
            early_hop(0, d, m).start()

    def early_reduce(k, m):
        for d in range(2):
            early_hop(k - 1, d, m).wait_recv()
            part = pm[d, m, owner_rows(d, k), :] + rm[d, k - 1, m].astype(F32)
            if k < hops:
                sm[d, k, m] = part.astype(BF16)
                early_hop(k, d, m).start()
            else:
                gate = part[:, :WIDTH].astype(BF16).astype(F32)
                up = part[:, WIDTH:].astype(BF16).astype(F32)
                hst[d, m] = (gate * jax.nn.sigmoid(gate) * up).astype(BF16)

    def later(step, *args):
        if args[-1] < EARLY:
            step(*args)

    for copy in local_w:
        copy.wait()
    for copy in swap_w:
        copy.wait_recv()
    product(0)
    early_product(0)
    give(0)
    reduce(1, 0)
    later(early_product, 1)
    reduce(2, 0)
    early_reduce(1, 0)
    reduce(3, 0)
    later(early_reduce, 1, 1)
    near_arrival(0).wait_recv()
    far(0).start()
    pair(1).start()
    near_arrival(1).wait_recv()
    far(1).start()
    pair(2).start()
    early_reduce(2, 0)
    product(1)
    product(2)
    give(1)
    give(2)
    later(early_reduce, 2, 1)
    reduce(1, 1)
    reduce(1, 2)
    early_reduce(3, 0)
    far_arrival(0).wait_recv()
    far_arrival(1).wait_recv()
    pair(3).start()
    reduce(2, 1)
    reduce(2, 2)
    product(3)
    give(3)
    later(early_product, 2)
    later(early_reduce, 3, 1)
    reduce(3, 1)
    reduce(3, 2)
    reduce(1, 3)
    later(early_reduce, 1, 2)
    reduce(2, 3)
    later(early_reduce, 2, 2)
    reduce(3, 3)
    later(early_reduce, 3, 2)

    for p in range(ny):
        for d in range(2):
            for i in range(1, nx):
                kv_arrival(d, p, i).wait_recv()
                kv_copy(d, p, i).wait_send()
            for k in range(hops):
                hop(k, d, p).wait_send()
        pair(p).wait_send()
        for copy in n_store(p):
            copy.wait()
        for copy in swap_mlp(p):
            copy.wait()
    for copy in swap_w:
        copy.wait_send()
    for m in range(EARLY):
        for copy in early_swap[m]:
            copy.wait_send()
        for d in range(2):
            for k in range(hops):
                early_hop(k, d, m).wait_send()
    for i in range(1, group):
        stat_copy(i).wait_send()
    to_south.wait_send()
    to_north.wait_send()
    far(0).wait_send()
    far(1).wait_send()
    stores = (pltpu.make_async_copy(qst, q_out, in_sem.at[0]), pltpu.make_async_copy(kv, kv_out, in_sem.at[1]),
              pltpu.make_async_copy(hst, h_out, in_sem.at[2]))
    for copy in stores:
        copy.start()
    for copy in stores:
        copy.wait()


def qkv_ring(x_blk, gain, cos, sin, wq, wk, wv, wg, wu, nx, ny):
    bt, feats = x_blk.shape
    tokens = bt * ny
    ob = bt // nx
    half = wg.shape[1] // CORES
    qhalf = wq.shape[1] // CORES
    cols = qhalf // 2 + HEAD
    hops = nx - 1
    any_spec = pl.BlockSpec(memory_space=pl.ANY)
    vmem = pl.BlockSpec(memory_space=pltpu.VMEM)
    dma = pltpu.SemaphoreType.DMA
    sds = jax.ShapeDtypeStruct
    return pl.pallas_call(
        functools.partial(qkv_kernel, nx, ny),
        out_shape=(sds((tokens, feats), BF16), sds((tokens, feats), BF16), sds((ny, ob, qhalf), BF16), sds((2, tokens, HEAD), BF16),
                   sds((feats, half), BF16), sds((feats, half), BF16), sds((2, EARLY, ob, WIDTH), BF16)),
        in_specs=[vmem] * 4 + [any_spec] * 5, out_specs=[any_spec] * 7,
        scratch_shapes=[
            pltpu.VMEM((tokens, feats), BF16), pltpu.VMEM((tokens, feats), BF16),
            pltpu.VMEM((2, 2 * feats, cols), BF16),
            pltpu.VMEM((2, nx, bt, cols), F32),
            pltpu.VMEM((2, hops, ny, ob, cols), BF16), pltpu.VMEM((2, hops, ny, ob, cols), BF16),
            pltpu.VMEM((ny, ob, qhalf), BF16), pltpu.VMEM((2, tokens, HEAD), BF16),
            pltpu.VMEM((2, EARLY, 2 * feats, 2 * WIDTH), BF16), pltpu.VMEM((2, EARLY, bt, 2 * WIDTH), F32),
            pltpu.VMEM((2, hops, EARLY, ob, 2 * WIDTH), BF16), pltpu.VMEM((2, hops, EARLY, ob, 2 * WIDTH), BF16),
            pltpu.VMEM((2, EARLY, ob, WIDTH), BF16),
            dma((EARLY, 2, 2)), dma((EARLY, 2, 2)), dma((EARLY, 2, 2)), dma((2, hops, EARLY)), dma((2, hops, EARLY)),
            pltpu.VMEM((nx * CORES, 8, bt), F32), dma((nx * CORES - 1,)), dma((nx * CORES - 1,)),
            dma((1 + 2 * ny,)), dma((4,)), dma((4,)), dma((4,)), dma((4,)), dma((4,)), dma((ny,)), dma((ny,)),
            dma((2, hops, ny)), dma((2, hops, ny)), dma((2, ny, hops)), dma((2, ny, hops)), dma((2, ny)), dma((2, ny)),
        ],
        compiler_params=pltpu.CompilerParams(collective_id=0, has_side_effects=True, vmem_limit_bytes=67043328),
        cost_estimate=pl.CostEstimate(flops=60_000_000_000, bytes_accessed=60_000_000, transcendentals=0),
    )(x_blk, gain, cos, sin, wq, wk, wv, wg, wu)


SLOTS = 3
HSLOTS = 8


def mlp_kernel(nx, ny, width, seq_len, nown_hbm, npar_hbm, q_hbm, kv_hbm, h_hbm, wg, wu, wgp, wup, wd, wo, out_ref, wdp, wop,
               nown, npar, wbuf, w2buf, pbuf, sbuf, rbuf, hid, acc, xrecv, ysend, yrecv, qst, kv, abuf, hst,
               in_sem, n_sem, w_sem, w2_sem, send_sem, recv_sem, xs_sem, xr_sem, ys_sem, yr_sem, gs_sem, gr_sem, credit, xcredit):
    tokens, feats = nown.shape
    bt = tokens // ny
    ob = bt // nx
    half = wgp.shape[1]
    dircols = half // 2
    ahalf = wop.shape[0]
    adir = ahalf // 2
    mlp_chunks = dircols // width
    chunks = mlp_chunks + adir // width
    total = ny * chunks
    last_hop = nx - 1
    kinds = 2 * last_hop
    tx = lax.axis_index("tx")
    ty = lax.axis_index("ty")
    core = lax.rem(tx, CORES)
    pos = tx // CORES
    partner = tx + 1 - 2 * core

    def target(d):
        return lax.rem(pos + 1 + d * (nx - 2), nx) * CORES + core

    def source(d):
        return lax.rem(pos + nx - 1 - d * (nx - 2), nx) * CORES + core

    def owner_rows(d, step):
        o = lax.rem(pos + (nx - 1 - step if d == 0 else 1 + step), nx)
        return pl.ds(pl.multiple_of(o * ob, ob), ob)

    def gather_rows(d, hops):
        o = lax.rem(pos + (nx - hops if d == 0 else hops), nx)
        return pl.ds(pl.multiple_of(o * ob, ob), ob)

    def block_rows(p):
        return pl.ds(pl.multiple_of(lax.rem(ty + 1 + p, ny) * bt, bt), bt)

    barrier = pltpu.get_barrier_semaphore()
    peers = [{"tx": partner}, {"tx": target(0)}, {"tx": target(1)}] + [{"ty": lax.rem(ty + k, ny)} for k in range(1, ny)]
    for peer in peers:
        pl.semaphore_signal(barrier, inc=1, device_id=peer, device_id_type=MESH)

    def w_copies(q, d):
        slot = lax.rem(q, 2)
        j = lax.rem(q, chunks)
        own = pl.ds(pl.multiple_of(core * half + d * dircols + j * width, width), width)
        par = pl.ds(pl.multiple_of(d * dircols + j * width, width), width)
        top, low = pl.ds(0, feats), pl.ds(feats, feats)
        left, right = pl.ds(0, width), pl.ds(width, width)
        dst = wbuf.at[slot, d]
        sem = w_sem.at[slot, d]
        return (pltpu.make_async_copy(wg.at[:, own], dst.at[top, left], sem.at[0]),
                pltpu.make_async_copy(wu.at[:, own], dst.at[top, right], sem.at[1]),
                pltpu.make_async_copy(wgp.at[:, par], dst.at[low, left], sem.at[2]),
                pltpu.make_async_copy(wup.at[:, par], dst.at[low, right], sem.at[3]))

    def w2_copies(q, d, mlp):
        slot = lax.rem(q, 2)
        j = lax.rem(q, chunks)
        dst = w2buf.at[slot]
        rows = pl.ds(d * width, width)
        sem = w2_sem.at[slot, d]
        if mlp:
            mine, theirs, size, first = wd, wdp, half, d * dircols + j * width
        else:
            mine, theirs, size, first = wo, wop, ahalf, d * adir + (j - mlp_chunks) * width
        own = pl.ds(pl.multiple_of(core * size + first, width), width)
        par = pl.ds(pl.multiple_of(first, width), width)
        return (pltpu.make_async_copy(mine.at[own, :], dst.at[0, rows, :], sem.at[0]),
                pltpu.make_async_copy(theirs.at[par, :], dst.at[1, rows, :], sem.at[1]))

    def w2_each(q, action):
        @pl.when(is_mlp(q))
        def _():
            for d in range(2):
                action(w2_copies(q, d, True))

        @pl.when(jnp.logical_not(is_mlp(q)))
        def _():
            for d in range(2):
                action(w2_copies(q, d, False))

    def start(copies):
        for copy in copies:
            copy.start()

    def wait(copies):
        for copy in copies:
            copy.wait()

    def hop(k, d, t):
        slot = lax.rem(t, SLOTS)
        if k < last_hop:
            src, dst = sbuf.at[d, k, slot], rbuf.at[d, k, slot]
        else:
            hslot = lax.rem(t - k + HSLOTS, HSLOTS)
            rows = gather_rows(d, k - last_hop)
            src = dst = hid.at[d, hslot, rows, :]
        return pltpu.make_async_remote_copy(src_ref=src, dst_ref=dst, send_sem=send_sem.at[d, k, slot],
                                            recv_sem=recv_sem.at[d, k, slot], device_id={"tx": target(d)}, device_id_type=MESH)

    def arrival(k, d, t):
        slot = lax.rem(t - 1 + SLOTS, SLOTS)
        if k < last_hop:
            dst = rbuf.at[d, k, slot]
        else:
            hslot = lax.rem(t - 1 - k + HSLOTS, HSLOTS)
            dst = hid.at[d, hslot, gather_rows(d, k - last_hop + 1), :]
        pltpu.make_async_remote_copy(src_ref=dst, dst_ref=dst, send_sem=send_sem.at[d, k, slot], recv_sem=recv_sem.at[d, k, slot],
                                     device_id={"tx": target(d)}, device_id_type=MESH).wait_recv()

    def valid(q):
        return jnp.logical_and(q >= 0, q < total)

    def is_mlp(q):
        return lax.rem(q, chunks) < mlp_chunks

    def reduces(q):
        early = jnp.logical_and(q >= total - chunks, q < total - chunks + EARLY)
        return jnp.logical_and(jnp.logical_and(valid(q), is_mlp(q)), jnp.logical_not(early))

    def n_copies(p):
        rows = block_rows(p)
        return (pltpu.make_async_copy(nown_hbm.at[rows, :], nown.at[rows, :], n_sem.at[0, p]),
                pltpu.make_async_copy(npar_hbm.at[rows, :], npar.at[rows, :], n_sem.at[1, p]))

    start(n_copies(0))
    for d in range(2):
        start(w_copies(0, d))
    loads = (pltpu.make_async_copy(q_hbm, qst, in_sem.at[0]), pltpu.make_async_copy(kv_hbm, kv, in_sem.at[1]),
             pltpu.make_async_copy(h_hbm, hst, in_sem.at[2]))
    pl.semaphore_wait(barrier, len(peers))
    swaps = []
    for i, (src, dst, size) in enumerate(((wd, wdp, half), (wo, wop, ahalf))):
        rows = pl.ds(pl.multiple_of((1 - core) * size, width), size)
        swaps.append(pltpu.make_async_remote_copy(src_ref=src.at[rows, :], dst_ref=dst, send_sem=gs_sem.at[i], recv_sem=gr_sem.at[i],
                                                  device_id={"tx": partner}, device_id_type=MESH))

    def attention(p):
        block = lax.rem(ty + 1 + p, ny)
        first = block * bt
        key0 = pl.multiple_of(first // seq_len * seq_len, seq_len)
        keys = kv[0, pl.ds(key0, seq_len), :]
        vals = kv[1, pl.ds(key0, seq_len), :]
        group = 4
        shape = (group * ob, seq_len)
        gap = (first + pos * ob + lax.rem(lax.broadcasted_iota(jnp.int32, shape, 0), ob)
               - key0 - lax.broadcasted_iota(jnp.int32, shape, 1))
        allowed = jnp.logical_and(gap >= 0, gap < WINDOW)
        for g in range(ahalf // HEAD // group):
            cols = [slice((g * group + h) * HEAD, (g * group + h + 1) * HEAD) for h in range(group)]
            queries = jnp.concatenate([qst[block, :, c] for c in cols], axis=0)
            scores = lax.dot_general(queries, keys, (((1,), (1,)), ((), ())), preferred_element_type=F32) * HEAD ** -0.5
            scores = jnp.where(allowed, scores, -1e30)
            weights = jnp.exp(scores - jnp.max(scores, axis=1, keepdims=True))
            norm = jnp.sum(weights, axis=1, keepdims=True)
            mixed = jnp.dot(weights.astype(BF16), vals, preferred_element_type=F32) / norm
            for h, c in enumerate(cols):
                abuf[:, c] = mixed[h * ob:(h + 1) * ob].astype(BF16)

    sends = total + kinds - 1
    signal_end = sends - SLOTS + 1

    def exchange_copy():
        return pltpu.make_async_remote_copy(src_ref=acc.at[1], dst_ref=xrecv, send_sem=xs_sem, recv_sem=xr_sem,
                                            device_id={"tx": partner}, device_id_type=MESH)

    def y_copy(p):
        return pltpu.make_async_remote_copy(src_ref=ysend.at[p], dst_ref=yrecv.at[p], send_sem=ys_sem.at[p], recv_sem=yr_sem.at[p],
                                            device_id={"ty": lax.rem(ty + 1 + p, ny)}, device_id_type=MESH)

    def tick(t, carry):
        @pl.when(jnp.logical_and(t >= SLOTS, t < sends))
        def _():
            for d in range(2):
                pl.semaphore_wait(credit.at[d], 1)

        for k in range(kinds):
            @pl.when((reduces if k < last_hop else valid)(t - SLOTS - k))
            def _():
                for d in range(2):
                    hop(k, d, t - SLOTS).wait_send()

        @pl.when(reduces(t + 1))
        def _():
            for d in range(2):
                start(w_copies(t + 1, d))

        @pl.when(jnp.logical_and(t < total, lax.rem(t, chunks) == 0))
        def _():
            wait(n_copies(t // chunks))

        @pl.when(reduces(t))
        def _():
            for d in range(2):
                wait(w_copies(t, d))

            rows = block_rows(t // chunks)
            slot = lax.rem(t, 2)
            pslot = lax.rem(t, nx)

            @pl.loop(0, 2)
            def _(d):
                pbuf[d, pslot] = (jnp.dot(nown[rows, :], wbuf[slot, d, :feats, :], preferred_element_type=F32)
                                  + jnp.dot(npar[rows, :], wbuf[slot, d, feats:, :], preferred_element_type=F32))
            for d in range(2):
                sbuf[d, 0, lax.rem(t, SLOTS)] = pbuf[d, pslot, owner_rows(d, 0), :].astype(BF16)
                hop(0, d, t).start()

        @pl.when(t == 1)
        def _():
            start(swaps)
            start(loads)
            for p in range(1, ny):
                start(n_copies(p))

        for k in range(1, last_hop + 1):
            @pl.when(reduces(t - k))
            def _():
                for d in range(2):
                    arrival(k - 1, d, t)
                    part = (pbuf[d, lax.rem(t - k + nx, nx), owner_rows(d, k), :]
                            + rbuf[d, k - 1, lax.rem(t - 1 + SLOTS, SLOTS)].astype(F32))
                    if k < last_hop:
                        sbuf[d, k, lax.rem(t, SLOTS)] = part.astype(BF16)
                    else:
                        gate = part[:, :width].astype(BF16).astype(F32)
                        up = part[:, width:].astype(BF16).astype(F32)
                        hslot = lax.rem(t - k + HSLOTS, HSLOTS)
                        hid[d, hslot, gather_rows(d, 0), :] = (gate * jax.nn.sigmoid(gate) * up).astype(BF16)
                    hop(k, d, t).start()

        for i in range(EARLY):
            @pl.when(t - last_hop == total - chunks + i)
            def _():
                for d in range(2):
                    hid[d, lax.rem(t - last_hop + HSLOTS, HSLOTS), gather_rows(d, 0), :] = hst[d, i]
                    hop(last_hop, d, t).start()

        for i in range(adir // width):
            q = t - last_hop

            @pl.when(jnp.logical_and(valid(q), lax.rem(q, chunks) == mlp_chunks + i))
            def _():
                for d in range(2):
                    hslot = lax.rem(q + HSLOTS, HSLOTS)
                    hid[d, hslot, gather_rows(d, 0), :] = abuf[:, d * adir + i * width:d * adir + (i + 1) * width]
                    hop(last_hop, d, t).start()

        for k in range(last_hop + 1, kinds):
            @pl.when(valid(t - k))
            def _():
                for d in range(2):
                    arrival(k - 1, d, t)
                    hop(k, d, t).start()

        q = t - kinds

        prev = q - 1

        @pl.when(jnp.logical_and(valid(prev), lax.rem(prev + 1, chunks) == 0))
        def _():
            p = prev // chunks
            copy = exchange_copy()
            copy.wait()

            @pl.when(p < ny - 1)
            def _():
                ysend[p] = (acc[0] + xrecv[...]).astype(BF16)
                pl.semaphore_signal(xcredit, inc=1, device_id={"tx": partner}, device_id_type=MESH)
                y_copy(p).start()

            @pl.when(p == ny - 1)
            def _():
                out = acc[0] + xrecv[...]
                for i in range(ny - 1):
                    y_copy(i).wait_recv()
                    out += yrecv[i].astype(F32)
                acc[0] = out

        @pl.when(valid(q))
        def _():
            p = q // chunks

            @pl.when(lax.rem(q, chunks) == 0)
            def _():
                acc[...] = jnp.zeros_like(acc)

            w2_each(q, wait)
            for d in range(2):
                arrival(kinds - 1, d, t)

            hslot = lax.rem(q, HSLOTS)
            slot = lax.rem(q, 2)

            @pl.loop(0, 2)
            def _(o):
                acc[o] += (jnp.dot(hid[0, hslot], w2buf[slot, o, :width, :], preferred_element_type=F32)
                           + jnp.dot(hid[1, hslot], w2buf[slot, o, width:, :], preferred_element_type=F32))

            @pl.when(lax.rem(q + 1, chunks) == 0)
            def _():
                @pl.when(p > 0)
                def _():
                    pl.semaphore_wait(xcredit, 1)
                exchange_copy().start()

        @pl.when(q + 1 == 0)
        def _():
            for copy in swaps:
                copy.wait_recv()

        @pl.when(valid(q + 1))
        def _():
            w2_each(q + 1, start)

        @pl.when(jnp.logical_and(t < total, lax.rem(t, chunks) == chunks // 2))
        def _():
            @pl.when(t < chunks)
            def _():
                wait(loads)
            attention(t // chunks)

        @pl.when(jnp.logical_and(t >= 1, t < signal_end))
        def _():
            for d in range(2):
                pl.semaphore_signal(credit.at[d], inc=1, device_id={"tx": source(d)}, device_id_type=MESH)
        return carry

    lax.fori_loop(0, total + kinds - 1 + SLOTS, tick, 0)
    for i in range(ny - 1):
        y_copy(i).wait_send()
    for copy in swaps:
        copy.wait_send()
    store = pltpu.make_async_copy(acc.at[0], out_ref, in_sem.at[0])
    store.start()
    store.wait()


def mlp_ring(n_own, n_par, q, kv, early, wg, wu, wgp, wup, wd, wo, nx, ny, width, seq_len):
    tokens, feats = n_own.shape
    bt = tokens // ny
    ob = bt // nx
    cols = wd.shape[1]
    half = wgp.shape[1]
    ahalf = wo.shape[0] // CORES
    kinds = 2 * (nx - 1)
    any_spec = pl.BlockSpec(memory_space=pl.ANY)
    dma = pltpu.SemaphoreType.DMA
    sds = jax.ShapeDtypeStruct
    return pl.pallas_call(
        functools.partial(mlp_kernel, nx, ny, width, seq_len),
        out_shape=(sds((bt, cols), F32), sds((half, cols), BF16), sds((ahalf, cols), BF16)),
        in_specs=[any_spec] * 11, out_specs=[any_spec] * 3,
        scratch_shapes=[
            pltpu.VMEM((tokens, feats), BF16),
            pltpu.VMEM((tokens, feats), BF16),
            pltpu.VMEM((2, 2, 2 * feats, 2 * width), BF16),
            pltpu.VMEM((2, 2, 2 * width, cols), BF16),
            pltpu.VMEM((2, nx, bt, 2 * width), F32),
            pltpu.VMEM((2, nx - 1, SLOTS, ob, 2 * width), BF16),
            pltpu.VMEM((2, nx - 1, SLOTS, ob, 2 * width), BF16),
            pltpu.VMEM((2, HSLOTS, bt, width), BF16),
            pltpu.VMEM((2, bt, cols), F32),
            pltpu.VMEM((bt, cols), F32),
            pltpu.VMEM((ny - 1, bt, cols), BF16),
            pltpu.VMEM((ny - 1, bt, cols), BF16),
            pltpu.VMEM(q.shape, BF16), pltpu.VMEM(kv.shape, BF16), pltpu.VMEM((ob, ahalf), BF16), pltpu.VMEM(early.shape, BF16),
            dma((3,)), dma((2, ny)), dma((2, 2, 4)), dma((2, 2, 2)),
            dma((2, kinds, SLOTS)), dma((2, kinds, SLOTS)),
            dma, dma, dma((ny - 1,)), dma((ny - 1,)), dma((2,)), dma((2,)),
            pltpu.SemaphoreType.REGULAR((2,)), pltpu.SemaphoreType.REGULAR,
        ],
        compiler_params=pltpu.CompilerParams(collective_id=1, has_side_effects=True, vmem_limit_bytes=67043328),
        cost_estimate=pl.CostEstimate(flops=400_000_000_000, bytes_accessed=200_000_000, transcendentals=0),
    )(n_own, n_par, q, kv, early, wg, wu, wgp, wup, wd, wo)


def solution(mesh):
    tx_size = mesh.shape["tx"]
    ty_size = mesh.shape["ty"]
    nx = tx_size // CORES

    def per_device(x_blk, positions, norm_gain, w_q, w_k, w_v, w_o, w_gate, w_up, w_down):
        seq_len = positions.shape[1]
        inv_freq = ROPE_THETA ** (-2.0 * (jnp.arange(HEAD) // 2).astype(F32) / HEAD)
        own_pos = positions.reshape(ty_size, nx, -1)
        own_pos = lax.dynamic_index_in_dim(own_pos, lax.axis_index("tx") // CORES, 1, keepdims=False)
        angle = own_pos.astype(F32)[:, :, None] * inv_freq
        cos = jnp.cos(angle)
        sin = jnp.sin(angle) * jnp.where(jnp.arange(HEAD) % 2 == 0, -1.0, 1.0).astype(F32)
        n_own, n_par, q, kv, wgp, wup, early = qkv_ring(x_blk, norm_gain[None, :], cos, sin, w_q, w_k, w_v, w_gate, w_up, nx, ty_size)
        block_sum, _, _ = mlp_ring(n_own, n_par, q, kv, early, w_gate, w_up, wgp, wup, w_down, w_o, nx, ty_size, WIDTH, seq_len)
        return (x_blk.astype(F32) + block_sum).astype(BF16)

    in_specs = (P(("dp", "ty"), "tx"), P("dp", None), P("tx"), P("tx", "ty"), P("tx", "ty"), P("tx", "ty"),
                P("ty", "tx"), P("tx", "ty"), P("tx", "ty"), P("ty", "tx"))
    return jax.shard_map(per_device, mesh=mesh, in_specs=in_specs, out_specs=P(("dp", "ty"), "tx"), check_vma=False)
```

```python
import functools
import jax
import jax.numpy as jnp
from jax import lax
from jax.experimental import pallas as pl
from jax.experimental.pallas import tpu as pltpu
from jax.sharding import PartitionSpec as P

HEAD = 128
WINDOW = 4096
ROPE_THETA = 50000
CORES = 2
WIDTH = 256
EARLY = 3
MESH = pl.DeviceIdType.MESH
F32 = jnp.float32
BF16 = jnp.bfloat16


def swap_lanes(x):
    width = x.shape[1]
    even = lax.rem(lax.broadcasted_iota(jnp.int32, x.shape, 1), 2) == 0
    return jnp.where(even, pltpu.roll(x, width - 1, 1), pltpu.roll(x, 1, 1))


def qkv_kernel(nx, ny, x_ref, gain_ref, cos_ref, sin_ref, wq, wk, wv, wg, wu, nown_out, npar_out, q_out, kv_out, wgp, wup, h_out,
               nown, npar, wbuf, pbuf, sbuf, rbuf, qst, kv, wm, pm, sm, rm, hst, wl_sem, wms_sem, wmr_sem, ms_sem, mr_sem, stats, st_sem, sr_sem, in_sem, w_sem, ws_sem, wr_sem, ns_sem, nr_sem, ps_sem, pr_sem,
               send_sem, recv_sem, ks_sem, kr_sem, gs_sem, gr_sem):
    tokens, feats = nown.shape
    bt = tokens // ny
    hb = bt // 2
    ob = bt // nx
    half = wgp.shape[1]
    qcols = wq.shape[1] // CORES // 2
    hops = nx - 1
    order = (0, 1, 3, 2)
    tx = lax.axis_index("tx")
    ty = lax.axis_index("ty")
    core = lax.rem(tx, CORES)
    pos = tx // CORES
    partner = tx + 1 - 2 * core
    north, south = lax.rem(ty + 1, ny), lax.rem(ty + ny - 1, ny)

    def chip(i):
        return lax.rem(pos + i, nx) * CORES + core

    def owner_rows(d, step):
        o = lax.rem(pos + (nx - 1 - step if d == 0 else 1 + step), nx)
        return pl.ds(pl.multiple_of(o * ob, ob), ob)

    def rows_of(off):
        return pl.ds(pl.multiple_of(lax.rem(ty + off, ny) * bt, bt), bt)

    def half_rows(off, i):
        return pl.ds(pl.multiple_of(lax.rem(ty + off, ny) * bt + i * hb, hb), hb)

    def remote(src, dst, send, recv, device):
        return pltpu.make_async_remote_copy(src_ref=src, dst_ref=dst, send_sem=send, recv_sem=recv, device_id=device, device_id_type=MESH)

    barrier = pltpu.get_barrier_semaphore()
    group = nx * CORES
    peers = [{"tx": lax.rem(tx + i, group)} for i in range(1, group)] + [{"ty": lax.rem(ty + k, ny)} for k in range(1, ny)]
    for peer in peers:
        pl.semaphore_signal(barrier, inc=1, device_id=peer, device_id_type=MESH)

    def w_parts(c):
        parts = []
        for d in range(2):
            col = pl.ds(pl.multiple_of(c * 2 * qcols + d * qcols, 128), qcols)
            small = pl.ds(pl.multiple_of(c * HEAD, HEAD), HEAD)
            parts.append((wq.at[:, col], d, pl.ds(0, qcols)))
            parts.append(((wk if d == 0 else wv).at[:, small], d, pl.ds(qcols, HEAD)))
        return parts

    def early_parts(c, m):
        for d in range(2):
            col = pl.ds(pl.multiple_of(c * half + d * (half // 2) + m * WIDTH, WIDTH), WIDTH)
            for i, src in enumerate((wg, wu)):
                yield src.at[:, col], d, i, pl.ds(i * WIDTH, WIDTH)

    local_w = [pltpu.make_async_copy(s, wbuf.at[d, pl.ds(0, feats), cols], w_sem.at[i]) for i, (s, d, cols) in enumerate(w_parts(core))]
    for copy in local_w:
        copy.start()

    x_wide = x_ref[...].astype(F32)
    part_mean = jnp.sum(x_wide, axis=1, keepdims=True) / feats
    centred = x_wide - part_mean
    lane = lax.broadcasted_iota(jnp.int32, (bt, HEAD), 1)
    stats[tx] = jnp.where(lane == 0, part_mean, jnp.sum(centred * centred, axis=1, keepdims=True)).T[:8]

    def stat_copy(i):
        return remote(stats.at[tx], stats.at[tx], st_sem.at[i - 1], sr_sem.at[i - 1], {"tx": lax.rem(tx + i, group)})

    def stat_arrival(i):
        slot = stats.at[lax.rem(tx + group - i, group)]
        return remote(slot, slot, st_sem.at[i - 1], sr_sem.at[i - 1], {"tx": lax.rem(tx + i, group)})

    pl.semaphore_wait(barrier, len(peers))
    for i in range(1, group):
        stat_copy(i).start()
    own = nown.at[rows_of(0), :]
    swap_w = [remote(s, wbuf.at[d, pl.ds(feats, feats), cols], ws_sem.at[i], wr_sem.at[i], {"tx": partner})
              for i, (s, d, cols) in enumerate(w_parts(1 - core))]
    for copy in swap_w:
        copy.start()
    for i in range(1, group):
        stat_arrival(i).wait_recv()
    means = [stats[i, 0:1, :] for i in range(group)]
    mean = sum(means) / group
    var = sum(stats[i, 1:2, :] + feats * (means[i] - mean) * (means[i] - mean) for i in range(group)) / (feats * group)
    sub = lax.broadcasted_iota(jnp.int32, (HEAD, bt), 0)
    cols = jnp.where(sub == 0, mean, lax.rsqrt(var + 1e-5)).T
    nown[rows_of(0), :] = (gain_ref[...] * (x_wide - cols[:, 0:1]) * cols[:, 1:2]).astype(BF16)
    to_south = remote(own, own, ns_sem.at[0], nr_sem.at[0], {"ty": south})
    to_north = remote(own, own, ns_sem.at[1], nr_sem.at[1], {"ty": north})
    to_south.start()
    to_north.start()

    early_local = [[pltpu.make_async_copy(src, wm.at[d, m, pl.ds(0, feats), cols], wl_sem.at[m, d, i])
                    for src, d, i, cols in early_parts(core, m)] for m in range(EARLY)]
    early_swap = [[remote(src, wm.at[d, m, pl.ds(feats, feats), cols], wms_sem.at[m, d, i], wmr_sem.at[m, d, i], {"tx": partner})
                   for src, d, i, cols in early_parts(1 - core, m)] for m in range(EARLY)]

    def pair(p):
        rows = rows_of(order[p])
        return remote(nown.at[rows, :], npar.at[rows, :], ps_sem.at[p], pr_sem.at[p], {"tx": partner})

    def far(i):
        rows = half_rows(1 if i == 0 else ny - 1, i)
        return remote(nown.at[rows, :], nown.at[rows, :], ns_sem.at[2 + i], nr_sem.at[2 + i], {"ty": south if i == 0 else north})

    def far_arrival(i):
        rows = half_rows(2, i)
        return remote(nown.at[rows, :], nown.at[rows, :], ns_sem.at[2 + i], nr_sem.at[2 + i], {"ty": south if i == 0 else north})

    def near_arrival(i):
        rows = rows_of(1 if i == 0 else ny - 1)
        return remote(nown.at[rows, :], nown.at[rows, :], ns_sem.at[i], nr_sem.at[i], {"ty": south if i == 0 else north})

    pair(0).start()
    for m in range(EARLY):
        for copy in early_local[m] + early_swap[m]:
            copy.start()

    piece = feats // ny
    goff = pl.multiple_of((1 - core) * half, 128)

    def swap_mlp(i):
        rows = pl.ds(i * piece, piece)
        return [remote(src.at[rows, pl.ds(goff, half)], dst.at[rows, :], gs_sem.at[k, i], gr_sem.at[k, i], {"tx": partner})
                for k, (src, dst) in enumerate(((wg, wgp), (wu, wup)))]

    def hop(k, d, p):
        target = chip(1 if d == 0 else nx - 1)
        return remote(sbuf.at[d, k, p], rbuf.at[d, k, p], send_sem.at[d, k, p], recv_sem.at[d, k, p], {"tx": target})

    def kv_rows(p):
        return pl.ds(pl.multiple_of(lax.rem(ty + order[p], ny) * bt + pos * ob, ob), ob)

    def kv_copy(d, p, i):
        rows = kv_rows(p)
        return remote(kv.at[d, rows, :], kv.at[d, rows, :], ks_sem.at[d, p, i - 1], kr_sem.at[d, p, i - 1], {"tx": chip(i)})

    def kv_arrival(d, p, i):
        rows = pl.ds(pl.multiple_of(lax.rem(ty + order[p], ny) * bt + lax.rem(pos + nx - i, nx) * ob, ob), ob)
        return remote(kv.at[d, rows, :], kv.at[d, rows, :], ks_sem.at[d, p, i - 1], kr_sem.at[d, p, i - 1], {"tx": chip(i)})

    def n_store(p):
        rows = rows_of(order[p])
        return (pltpu.make_async_copy(nown.at[rows, :], nown_out.at[rows, :], in_sem.at[1 + 2 * p]),
                pltpu.make_async_copy(npar.at[rows, :], npar_out.at[rows, :], in_sem.at[2 + 2 * p]))

    def product(p):
        pair(p).wait_recv()
        for copy in n_store(p):
            copy.start()
        rows = rows_of(order[p])

        @pl.loop(0, 2)
        def _(d):
            pbuf[d, p] = (jnp.dot(nown[rows, :], wbuf[d, :feats, :], preferred_element_type=F32)
                          + jnp.dot(npar[rows, :], wbuf[d, feats:, :], preferred_element_type=F32))
        for d in range(2):
            sbuf[d, 0, p] = pbuf[d, p, owner_rows(d, 0), :].astype(BF16)
            hop(0, d, p).start()

    def reduce(k, p):
        for d in range(2):
            hop(k - 1, d, p).wait_recv()
            part = pbuf[d, p, owner_rows(d, k), :] + rbuf[d, k - 1, p].astype(F32)
            if k < hops:
                sbuf[d, k, p] = part.astype(BF16)
                hop(k, d, p).start()
                continue
            rows = kv_rows(p)
            block = lax.rem(ty + order[p], ny)
            part = part.astype(BF16).astype(F32)
            cos, sin = cos_ref[block], sin_ref[block]
            small = part[:, qcols:]
            if d == 0:
                small = small * cos + swap_lanes(small) * sin
            kv[d, rows, :] = small.astype(BF16)
            for i in range(1, nx):
                kv_copy(d, p, i).start()
            for h in range(qcols // HEAD):
                head = part[:, h * HEAD:(h + 1) * HEAD]
                qst[block, :, d * qcols + h * HEAD:d * qcols + (h + 1) * HEAD] = (head * cos + swap_lanes(head) * sin).astype(BF16)

    def give(i):
        for copy in swap_mlp(i):
            copy.start()

    def early_hop(k, d, m):
        target = chip(1 if d == 0 else nx - 1)
        return remote(sm.at[d, k, m], rm.at[d, k, m], ms_sem.at[d, k, m], mr_sem.at[d, k, m], {"tx": target})

    def early_product(m):
        for copy in early_local[m]:
            copy.wait()
        for copy in early_swap[m]:
            copy.wait_recv()
        rows = rows_of(0)

        @pl.loop(0, 2)
        def _(d):
            pm[d, m] = (jnp.dot(nown[rows, :], wm[d, m, :feats, :], preferred_element_type=F32)
                        + jnp.dot(npar[rows, :], wm[d, m, feats:, :], preferred_element_type=F32))
        for d in range(2):
            sm[d, 0, m] = pm[d, m, owner_rows(d, 0), :].astype(BF16)
            early_hop(0, d, m).start()

    def early_reduce(k, m):
        for d in range(2):
            early_hop(k - 1, d, m).wait_recv()
            part = pm[d, m, owner_rows(d, k), :] + rm[d, k - 1, m].astype(F32)
            if k < hops:
                sm[d, k, m] = part.astype(BF16)
                early_hop(k, d, m).start()
            else:
                gate = part[:, :WIDTH].astype(BF16).astype(F32)
                up = part[:, WIDTH:].astype(BF16).astype(F32)
                hst[d, m] = (gate * jax.nn.sigmoid(gate) * up).astype(BF16)

    def later(step, *args):
        if args[-1] < EARLY:
            step(*args)

    for copy in local_w:
        copy.wait()
    for copy in swap_w:
        copy.wait_recv()
    product(0)
    early_product(0)
    give(0)
    reduce(1, 0)
    later(early_product, 1)
    reduce(2, 0)
    early_reduce(1, 0)
    later(early_reduce, 1, 1)
    near_arrival(0).wait_recv()
    far(0).start()
    pair(1).start()
    near_arrival(1).wait_recv()
    far(1).start()
    pair(2).start()
    early_reduce(2, 0)
    reduce(3, 0)
    product(1)
    product(2)
    give(1)
    give(2)
    later(early_reduce, 2, 1)
    reduce(1, 1)
    reduce(1, 2)
    early_reduce(3, 0)
    far_arrival(0).wait_recv()
    far_arrival(1).wait_recv()
    pair(3).start()
    reduce(2, 1)
    reduce(2, 2)
    product(3)
    give(3)
    later(early_product, 2)
    later(early_reduce, 3, 1)
    reduce(3, 1)
    reduce(3, 2)
    reduce(1, 3)
    later(early_reduce, 1, 2)
    reduce(2, 3)
    later(early_reduce, 2, 2)
    reduce(3, 3)
    later(early_reduce, 3, 2)

    for p in range(ny):
        for d in range(2):
            for i in range(1, nx):
                kv_arrival(d, p, i).wait_recv()
                kv_copy(d, p, i).wait_send()
            for k in range(hops):
                hop(k, d, p).wait_send()
        pair(p).wait_send()
        for copy in n_store(p):
            copy.wait()
        for copy in swap_mlp(p):
            copy.wait()
    for copy in swap_w:
        copy.wait_send()
    for m in range(EARLY):
        for copy in early_swap[m]:
            copy.wait_send()
        for d in range(2):
            for k in range(hops):
                early_hop(k, d, m).wait_send()
    for i in range(1, group):
        stat_copy(i).wait_send()
    to_south.wait_send()
    to_north.wait_send()
    far(0).wait_send()
    far(1).wait_send()
    stores = (pltpu.make_async_copy(qst, q_out, in_sem.at[0]), pltpu.make_async_copy(kv, kv_out, in_sem.at[1]),
              pltpu.make_async_copy(hst, h_out, in_sem.at[2]))
    for copy in stores:
        copy.start()
    for copy in stores:
        copy.wait()


def qkv_ring(x_blk, gain, cos, sin, wq, wk, wv, wg, wu, nx, ny):
    bt, feats = x_blk.shape
    tokens = bt * ny
    ob = bt // nx
    half = wg.shape[1] // CORES
    qhalf = wq.shape[1] // CORES
    cols = qhalf // 2 + HEAD
    hops = nx - 1
    any_spec = pl.BlockSpec(memory_space=pl.ANY)
    vmem = pl.BlockSpec(memory_space=pltpu.VMEM)
    dma = pltpu.SemaphoreType.DMA
    sds = jax.ShapeDtypeStruct
    return pl.pallas_call(
        functools.partial(qkv_kernel, nx, ny),
        out_shape=(sds((tokens, feats), BF16), sds((tokens, feats), BF16), sds((ny, ob, qhalf), BF16), sds((2, tokens, HEAD), BF16),
                   sds((feats, half), BF16), sds((feats, half), BF16), sds((2, EARLY, ob, WIDTH), BF16)),
        in_specs=[vmem] * 4 + [any_spec] * 5, out_specs=[any_spec] * 7,
        scratch_shapes=[
            pltpu.VMEM((tokens, feats), BF16), pltpu.VMEM((tokens, feats), BF16),
            pltpu.VMEM((2, 2 * feats, cols), BF16),
            pltpu.VMEM((2, nx, bt, cols), F32),
            pltpu.VMEM((2, hops, ny, ob, cols), BF16), pltpu.VMEM((2, hops, ny, ob, cols), BF16),
            pltpu.VMEM((ny, ob, qhalf), BF16), pltpu.VMEM((2, tokens, HEAD), BF16),
            pltpu.VMEM((2, EARLY, 2 * feats, 2 * WIDTH), BF16), pltpu.VMEM((2, EARLY, bt, 2 * WIDTH), F32),
            pltpu.VMEM((2, hops, EARLY, ob, 2 * WIDTH), BF16), pltpu.VMEM((2, hops, EARLY, ob, 2 * WIDTH), BF16),
            pltpu.VMEM((2, EARLY, ob, WIDTH), BF16),
            dma((EARLY, 2, 2)), dma((EARLY, 2, 2)), dma((EARLY, 2, 2)), dma((2, hops, EARLY)), dma((2, hops, EARLY)),
            pltpu.VMEM((nx * CORES, 8, bt), F32), dma((nx * CORES - 1,)), dma((nx * CORES - 1,)),
            dma((1 + 2 * ny,)), dma((4,)), dma((4,)), dma((4,)), dma((4,)), dma((4,)), dma((ny,)), dma((ny,)),
            dma((2, hops, ny)), dma((2, hops, ny)), dma((2, ny, hops)), dma((2, ny, hops)), dma((2, ny)), dma((2, ny)),
        ],
        compiler_params=pltpu.CompilerParams(collective_id=0, has_side_effects=True, vmem_limit_bytes=67043328),
        cost_estimate=pl.CostEstimate(flops=60_000_000_000, bytes_accessed=60_000_000, transcendentals=0),
    )(x_blk, gain, cos, sin, wq, wk, wv, wg, wu)


SLOTS = 3
HSLOTS = 8


def mlp_kernel(nx, ny, width, seq_len, nown_hbm, npar_hbm, q_hbm, kv_hbm, h_hbm, wg, wu, wgp, wup, wd, wo, out_ref, wdp, wop,
               nown, npar, wbuf, w2buf, pbuf, sbuf, rbuf, hid, acc, xrecv, ysend, yrecv, qst, kv, abuf, hst,
               in_sem, n_sem, w_sem, w2_sem, send_sem, recv_sem, xs_sem, xr_sem, ys_sem, yr_sem, gs_sem, gr_sem, credit, xcredit):
    tokens, feats = nown.shape
    bt = tokens // ny
    ob = bt // nx
    half = wgp.shape[1]
    dircols = half // 2
    ahalf = wop.shape[0]
    adir = ahalf // 2
    mlp_chunks = dircols // width
    chunks = mlp_chunks + adir // width
    total = ny * chunks
    last_hop = nx - 1
    kinds = 2 * last_hop
    tx = lax.axis_index("tx")
    ty = lax.axis_index("ty")
    core = lax.rem(tx, CORES)
    pos = tx // CORES
    partner = tx + 1 - 2 * core

    def target(d):
        return lax.rem(pos + 1 + d * (nx - 2), nx) * CORES + core

    def source(d):
        return lax.rem(pos + nx - 1 - d * (nx - 2), nx) * CORES + core

    def owner_rows(d, step):
        o = lax.rem(pos + (nx - 1 - step if d == 0 else 1 + step), nx)
        return pl.ds(pl.multiple_of(o * ob, ob), ob)

    def gather_rows(d, hops):
        o = lax.rem(pos + (nx - hops if d == 0 else hops), nx)
        return pl.ds(pl.multiple_of(o * ob, ob), ob)

    def block_rows(p):
        return pl.ds(pl.multiple_of(lax.rem(ty + 1 + p, ny) * bt, bt), bt)

    barrier = pltpu.get_barrier_semaphore()
    peers = [{"tx": partner}, {"tx": target(0)}, {"tx": target(1)}] + [{"ty": lax.rem(ty + k, ny)} for k in range(1, ny)]
    for peer in peers:
        pl.semaphore_signal(barrier, inc=1, device_id=peer, device_id_type=MESH)

    def w_copies(q, d):
        slot = lax.rem(q, 2)
        j = lax.rem(q, chunks)
        own = pl.ds(pl.multiple_of(core * half + d * dircols + j * width, width), width)
        par = pl.ds(pl.multiple_of(d * dircols + j * width, width), width)
        top, low = pl.ds(0, feats), pl.ds(feats, feats)
        left, right = pl.ds(0, width), pl.ds(width, width)
        dst = wbuf.at[slot, d]
        sem = w_sem.at[slot, d]
        return (pltpu.make_async_copy(wg.at[:, own], dst.at[top, left], sem.at[0]),
                pltpu.make_async_copy(wu.at[:, own], dst.at[top, right], sem.at[1]),
                pltpu.make_async_copy(wgp.at[:, par], dst.at[low, left], sem.at[2]),
                pltpu.make_async_copy(wup.at[:, par], dst.at[low, right], sem.at[3]))

    def w2_copies(q, d, mlp):
        slot = lax.rem(q, 2)
        j = lax.rem(q, chunks)
        dst = w2buf.at[slot]
        rows = pl.ds(d * width, width)
        sem = w2_sem.at[slot, d]
        if mlp:
            mine, theirs, size, first = wd, wdp, half, d * dircols + j * width
        else:
            mine, theirs, size, first = wo, wop, ahalf, d * adir + (j - mlp_chunks) * width
        own = pl.ds(pl.multiple_of(core * size + first, width), width)
        par = pl.ds(pl.multiple_of(first, width), width)
        return (pltpu.make_async_copy(mine.at[own, :], dst.at[0, rows, :], sem.at[0]),
                pltpu.make_async_copy(theirs.at[par, :], dst.at[1, rows, :], sem.at[1]))

    def w2_each(q, action):
        @pl.when(is_mlp(q))
        def _():
            for d in range(2):
                action(w2_copies(q, d, True))

        @pl.when(jnp.logical_not(is_mlp(q)))
        def _():
            for d in range(2):
                action(w2_copies(q, d, False))

    def start(copies):
        for copy in copies:
            copy.start()

    def wait(copies):
        for copy in copies:
            copy.wait()

    def hop(k, d, t):
        slot = lax.rem(t, SLOTS)
        if k < last_hop:
            src, dst = sbuf.at[d, k, slot], rbuf.at[d, k, slot]
        else:
            hslot = lax.rem(t - k + HSLOTS, HSLOTS)
            rows = gather_rows(d, k - last_hop)
            src = dst = hid.at[d, hslot, rows, :]
        return pltpu.make_async_remote_copy(src_ref=src, dst_ref=dst, send_sem=send_sem.at[d, k, slot],
                                            recv_sem=recv_sem.at[d, k, slot], device_id={"tx": target(d)}, device_id_type=MESH)

    def arrival(k, d, t):
        slot = lax.rem(t - 1 + SLOTS, SLOTS)
        if k < last_hop:
            dst = rbuf.at[d, k, slot]
        else:
            hslot = lax.rem(t - 1 - k + HSLOTS, HSLOTS)
            dst = hid.at[d, hslot, gather_rows(d, k - last_hop + 1), :]
        pltpu.make_async_remote_copy(src_ref=dst, dst_ref=dst, send_sem=send_sem.at[d, k, slot], recv_sem=recv_sem.at[d, k, slot],
                                     device_id={"tx": target(d)}, device_id_type=MESH).wait_recv()

    def valid(q):
        return jnp.logical_and(q >= 0, q < total)

    def is_mlp(q):
        return lax.rem(q, chunks) < mlp_chunks

    def reduces(q):
        early = jnp.logical_and(q >= total - chunks, q < total - chunks + EARLY)
        return jnp.logical_and(jnp.logical_and(valid(q), is_mlp(q)), jnp.logical_not(early))

    def n_copies(p):
        rows = block_rows(p)
        return (pltpu.make_async_copy(nown_hbm.at[rows, :], nown.at[rows, :], n_sem.at[0, p]),
                pltpu.make_async_copy(npar_hbm.at[rows, :], npar.at[rows, :], n_sem.at[1, p]))

    start(n_copies(0))
    for d in range(2):
        start(w_copies(0, d))
    loads = (pltpu.make_async_copy(q_hbm, qst, in_sem.at[0]), pltpu.make_async_copy(kv_hbm, kv, in_sem.at[1]),
             pltpu.make_async_copy(h_hbm, hst, in_sem.at[2]))
    pl.semaphore_wait(barrier, len(peers))
    swaps = []
    for i, (src, dst, size) in enumerate(((wd, wdp, half), (wo, wop, ahalf))):
        rows = pl.ds(pl.multiple_of((1 - core) * size, width), size)
        swaps.append(pltpu.make_async_remote_copy(src_ref=src.at[rows, :], dst_ref=dst, send_sem=gs_sem.at[i], recv_sem=gr_sem.at[i],
                                                  device_id={"tx": partner}, device_id_type=MESH))

    def attention(p):
        block = lax.rem(ty + 1 + p, ny)
        first = block * bt
        key0 = pl.multiple_of(first // seq_len * seq_len, seq_len)
        keys = kv[0, pl.ds(key0, seq_len), :]
        vals = kv[1, pl.ds(key0, seq_len), :]
        group = 4
        shape = (group * ob, seq_len)
        gap = (first + pos * ob + lax.rem(lax.broadcasted_iota(jnp.int32, shape, 0), ob)
               - key0 - lax.broadcasted_iota(jnp.int32, shape, 1))
        allowed = jnp.logical_and(gap >= 0, gap < WINDOW)
        for g in range(ahalf // HEAD // group):
            cols = [slice((g * group + h) * HEAD, (g * group + h + 1) * HEAD) for h in range(group)]
            queries = jnp.concatenate([qst[block, :, c] for c in cols], axis=0)
            scores = lax.dot_general(queries, keys, (((1,), (1,)), ((), ())), preferred_element_type=F32) * HEAD ** -0.5
            scores = jnp.where(allowed, scores, -1e30)
            weights = jnp.exp(scores - jnp.max(scores, axis=1, keepdims=True))
            norm = jnp.sum(weights, axis=1, keepdims=True)
            mixed = jnp.dot(weights.astype(BF16), vals, preferred_element_type=F32) / norm
            for h, c in enumerate(cols):
                abuf[:, c] = mixed[h * ob:(h + 1) * ob].astype(BF16)

    sends = total + kinds - 1
    signal_end = sends - SLOTS + 1

    def exchange_copy():
        return pltpu.make_async_remote_copy(src_ref=acc.at[1], dst_ref=xrecv, send_sem=xs_sem, recv_sem=xr_sem,
                                            device_id={"tx": partner}, device_id_type=MESH)

    def y_copy(p):
        return pltpu.make_async_remote_copy(src_ref=ysend.at[p], dst_ref=yrecv.at[p], send_sem=ys_sem.at[p], recv_sem=yr_sem.at[p],
                                            device_id={"ty": lax.rem(ty + 1 + p, ny)}, device_id_type=MESH)

    def tick(t, carry):
        @pl.when(jnp.logical_and(t >= SLOTS, t < sends))
        def _():
            for d in range(2):
                pl.semaphore_wait(credit.at[d], 1)

        for k in range(kinds):
            @pl.when((reduces if k < last_hop else valid)(t - SLOTS - k))
            def _():
                for d in range(2):
                    hop(k, d, t - SLOTS).wait_send()

        @pl.when(reduces(t + 1))
        def _():
            for d in range(2):
                start(w_copies(t + 1, d))

        @pl.when(jnp.logical_and(t < total, lax.rem(t, chunks) == 0))
        def _():
            wait(n_copies(t // chunks))

        @pl.when(reduces(t))
        def _():
            for d in range(2):
                wait(w_copies(t, d))

            rows = block_rows(t // chunks)
            slot = lax.rem(t, 2)
            pslot = lax.rem(t, nx)

            @pl.loop(0, 2)
            def _(d):
                pbuf[d, pslot] = (jnp.dot(nown[rows, :], wbuf[slot, d, :feats, :], preferred_element_type=F32)
                                  + jnp.dot(npar[rows, :], wbuf[slot, d, feats:, :], preferred_element_type=F32))
            for d in range(2):
                sbuf[d, 0, lax.rem(t, SLOTS)] = pbuf[d, pslot, owner_rows(d, 0), :].astype(BF16)
                hop(0, d, t).start()

        @pl.when(t == 1)
        def _():
            start(swaps)
            start(loads)
            for p in range(1, ny):
                start(n_copies(p))

        for k in range(1, last_hop + 1):
            @pl.when(reduces(t - k))
            def _():
                for d in range(2):
                    arrival(k - 1, d, t)
                    part = (pbuf[d, lax.rem(t - k + nx, nx), owner_rows(d, k), :]
                            + rbuf[d, k - 1, lax.rem(t - 1 + SLOTS, SLOTS)].astype(F32))
                    if k < last_hop:
                        sbuf[d, k, lax.rem(t, SLOTS)] = part.astype(BF16)
                    else:
                        gate = part[:, :width].astype(BF16).astype(F32)
                        up = part[:, width:].astype(BF16).astype(F32)
                        hslot = lax.rem(t - k + HSLOTS, HSLOTS)
                        hid[d, hslot, gather_rows(d, 0), :] = (gate * jax.nn.sigmoid(gate) * up).astype(BF16)
                    hop(k, d, t).start()

        for i in range(EARLY):
            @pl.when(t - last_hop == total - chunks + i)
            def _():
                for d in range(2):
                    hid[d, lax.rem(t - last_hop + HSLOTS, HSLOTS), gather_rows(d, 0), :] = hst[d, i]
                    hop(last_hop, d, t).start()

        for i in range(adir // width):
            q = t - last_hop

            @pl.when(jnp.logical_and(valid(q), lax.rem(q, chunks) == mlp_chunks + i))
            def _():
                for d in range(2):
                    hslot = lax.rem(q + HSLOTS, HSLOTS)
                    hid[d, hslot, gather_rows(d, 0), :] = abuf[:, d * adir + i * width:d * adir + (i + 1) * width]
                    hop(last_hop, d, t).start()

        for k in range(last_hop + 1, kinds):
            @pl.when(valid(t - k))
            def _():
                for d in range(2):
                    arrival(k - 1, d, t)
                    hop(k, d, t).start()

        q = t - kinds

        prev = q - 1

        @pl.when(jnp.logical_and(valid(prev), lax.rem(prev + 1, chunks) == 0))
        def _():
            p = prev // chunks
            copy = exchange_copy()
            copy.wait()

            @pl.when(p < ny - 1)
            def _():
                ysend[p] = (acc[0] + xrecv[...]).astype(BF16)
                pl.semaphore_signal(xcredit, inc=1, device_id={"tx": partner}, device_id_type=MESH)
                y_copy(p).start()

            @pl.when(p == ny - 1)
            def _():
                out = acc[0] + xrecv[...]
                for i in range(ny - 1):
                    y_copy(i).wait_recv()
                    out += yrecv[i].astype(F32)
                acc[0] = out

        @pl.when(valid(q))
        def _():
            p = q // chunks

            @pl.when(lax.rem(q, chunks) == 0)
            def _():
                acc[...] = jnp.zeros_like(acc)

            w2_each(q, wait)
            for d in range(2):
                arrival(kinds - 1, d, t)

            hslot = lax.rem(q, HSLOTS)
            slot = lax.rem(q, 2)

            @pl.loop(0, 2)
            def _(o):
                acc[o] += (jnp.dot(hid[0, hslot], w2buf[slot, o, :width, :], preferred_element_type=F32)
                           + jnp.dot(hid[1, hslot], w2buf[slot, o, width:, :], preferred_element_type=F32))

            @pl.when(lax.rem(q + 1, chunks) == 0)
            def _():
                @pl.when(p > 0)
                def _():
                    pl.semaphore_wait(xcredit, 1)
                exchange_copy().start()

        @pl.when(q + 1 == 0)
        def _():
            for copy in swaps:
                copy.wait_recv()

        @pl.when(valid(q + 1))
        def _():
            w2_each(q + 1, start)

        @pl.when(jnp.logical_and(t < total, lax.rem(t, chunks) == chunks // 2))
        def _():
            @pl.when(t < chunks)
            def _():
                wait(loads)
            attention(t // chunks)

        @pl.when(jnp.logical_and(t >= 1, t < signal_end))
        def _():
            for d in range(2):
                pl.semaphore_signal(credit.at[d], inc=1, device_id={"tx": source(d)}, device_id_type=MESH)
        return carry

    lax.fori_loop(0, total + kinds - 1 + SLOTS, tick, 0)
    for i in range(ny - 1):
        y_copy(i).wait_send()
    for copy in swaps:
        copy.wait_send()
    store = pltpu.make_async_copy(acc.at[0], out_ref, in_sem.at[0])
    store.start()
    store.wait()


def mlp_ring(n_own, n_par, q, kv, early, wg, wu, wgp, wup, wd, wo, nx, ny, width, seq_len):
    tokens, feats = n_own.shape
    bt = tokens // ny
    ob = bt // nx
    cols = wd.shape[1]
    half = wgp.shape[1]
    ahalf = wo.shape[0] // CORES
    kinds = 2 * (nx - 1)
    any_spec = pl.BlockSpec(memory_space=pl.ANY)
    dma = pltpu.SemaphoreType.DMA
    sds = jax.ShapeDtypeStruct
    return pl.pallas_call(
        functools.partial(mlp_kernel, nx, ny, width, seq_len),
        out_shape=(sds((bt, cols), F32), sds((half, cols), BF16), sds((ahalf, cols), BF16)),
        in_specs=[any_spec] * 11, out_specs=[any_spec] * 3,
        scratch_shapes=[
            pltpu.VMEM((tokens, feats), BF16),
            pltpu.VMEM((tokens, feats), BF16),
            pltpu.VMEM((2, 2, 2 * feats, 2 * width), BF16),
            pltpu.VMEM((2, 2, 2 * width, cols), BF16),
            pltpu.VMEM((2, nx, bt, 2 * width), F32),
            pltpu.VMEM((2, nx - 1, SLOTS, ob, 2 * width), BF16),
            pltpu.VMEM((2, nx - 1, SLOTS, ob, 2 * width), BF16),
            pltpu.VMEM((2, HSLOTS, bt, width), BF16),
            pltpu.VMEM((2, bt, cols), F32),
            pltpu.VMEM((bt, cols), F32),
            pltpu.VMEM((ny - 1, bt, cols), BF16),
            pltpu.VMEM((ny - 1, bt, cols), BF16),
            pltpu.VMEM(q.shape, BF16), pltpu.VMEM(kv.shape, BF16), pltpu.VMEM((ob, ahalf), BF16), pltpu.VMEM(early.shape, BF16),
            dma((3,)), dma((2, ny)), dma((2, 2, 4)), dma((2, 2, 2)),
            dma((2, kinds, SLOTS)), dma((2, kinds, SLOTS)),
            dma, dma, dma((ny - 1,)), dma((ny - 1,)), dma((2,)), dma((2,)),
            pltpu.SemaphoreType.REGULAR((2,)), pltpu.SemaphoreType.REGULAR,
        ],
        compiler_params=pltpu.CompilerParams(collective_id=1, has_side_effects=True, vmem_limit_bytes=67043328),
        cost_estimate=pl.CostEstimate(flops=400_000_000_000, bytes_accessed=200_000_000, transcendentals=0),
    )(n_own, n_par, q, kv, early, wg, wu, wgp, wup, wd, wo)


def solution(mesh):
    tx_size = mesh.shape["tx"]
    ty_size = mesh.shape["ty"]
    nx = tx_size // CORES

    def per_device(x_blk, positions, norm_gain, w_q, w_k, w_v, w_o, w_gate, w_up, w_down):
        seq_len = positions.shape[1]
        inv_freq = ROPE_THETA ** (-2.0 * (jnp.arange(HEAD) // 2).astype(F32) / HEAD)
        own_pos = positions.reshape(ty_size, nx, -1)
        own_pos = lax.dynamic_index_in_dim(own_pos, lax.axis_index("tx") // CORES, 1, keepdims=False)
        angle = own_pos.astype(F32)[:, :, None] * inv_freq
        cos = jnp.cos(angle)
        sin = jnp.sin(angle) * jnp.where(jnp.arange(HEAD) % 2 == 0, -1.0, 1.0).astype(F32)
        n_own, n_par, q, kv, wgp, wup, early = qkv_ring(x_blk, norm_gain[None, :], cos, sin, w_q, w_k, w_v, w_gate, w_up, nx, ty_size)
        block_sum, _, _ = mlp_ring(n_own, n_par, q, kv, early, w_gate, w_up, wgp, wup, w_down, w_o, nx, ty_size, WIDTH, seq_len)
        return (x_blk.astype(F32) + block_sum).astype(BF16)

    in_specs = (P(("dp", "ty"), "tx"), P("dp", None), P("tx"), P("tx", "ty"), P("tx", "ty"), P("tx", "ty"),
                P("ty", "tx"), P("tx", "ty"), P("tx", "ty"), P("ty", "tx"))
    return jax.shard_map(per_device, mesh=mesh, in_specs=in_specs, out_specs=P(("dp", "ty"), "tx"), check_vma=False)
```
